128 devices in a mesh: expert: 16 (over x_hi, y, core), row: 8 (over z, x_lo).
Axes of the slice: x: 4 (x_hi: 2, x_lo: 2; x = x_hi * 2 + x_lo), y: 4, z: 4, core: 2. Of those that a mesh axis runs over, the one named last changes fastest.
Arguments:
- weights: bfloat16 [16, 7168, 2048], P('expert', 'row'), may hold values from -6 to 6
- left_bits: int32 [16, 7168], P('expert', 'row'), may hold values from 0 to 1
- right_bits: int32 [16, 2048], P('expert'), may hold values from 0 to 1
- groups: int32 [16, 2048], P('expert'), may hold values from 0 to 15, never falling along the last dimension, each value on 1 to 256 neighbouring positions
Outputs:
- scaled: bfloat16 [16, 7168, 2048], P('expert', 'row')
- block_error: float32 [16, 7168, 256], P('expert', 'row')
- scales: float32 [16, 16], P('expert')
- expert_error: float32 [16], P('expert')
- total_error: float32 [], replicated
The draws below stay inside these ranges and needn't reach their ends.
Inputs may be any that keep to these rules, and one draw needn't show every extreme that they name: Along each expert's 2048 columns the group number never falls; each of the 16 groups holds 1 to 256 columns.
All inputs are finite; a program needn't handle non-finite values.
Results may differ from the reference program's by a relative error of at most 0.0091.
Values may be sent and summed in bfloat16 or wider, within the bound.
A program may use at most 128 MiB of HBM per device.

```python
import math
import jax
import jax.numpy as jnp
import numpy as np
from jax import lax

D = 7168
FF = 2048
HB = 128
OUTER = 16
GROUPS = 16
BLOCKS = 56
GROUP_MOST = 256
EXPERTS = 16


def draw_weights(key, part):
    scale_key = jax.random.fold_in(key, 11)
    entry_key = jax.random.fold_in(key, 12)
    magnitude = jnp.exp(jax.random.uniform(scale_key, (EXPERTS, 1, 1), jnp.float32, math.log(0.02), math.log(1.0)))
    entries = jnp.clip(jax.random.normal(entry_key, (EXPERTS, D, FF), jnp.float32), -6.0, 6.0)
    return jnp.clip(entries * magnitude, -6.0, 6.0).astype(jnp.bfloat16)


def place_ends(result, stream_key, low, high):
    longest = result.shape.index(max(result.shape))
    spots = []
    for shift in (0, 1):
        where = [jax.random.randint(jax.random.fold_in(stream_key, axis), (), 0, length) for axis, length in enumerate(result.shape)]
        where[longest] = (where[longest] + shift) % result.shape[longest]
        spots.append(tuple(where))
    return result.at[spots[0]].set(low).at[spots[1]].set(high)


def profile(number_of, total, most, slope):
    loads = [(1 << 20) // math.isqrt(grade ** slope) + 1 for grade in range(2, number_of + 1)]
    spare, holding = total - most - (number_of - 1), [1] * (number_of - 1)
    while spare > 0:
        free = [i for i in range(number_of - 1) if holding[i] < most]
        whole, left = sum([loads[i] for i in free]), spare
        for i in free:
            more = min(most - holding[i], max(1, left * loads[i] // whole), spare)
            holding[i] = holding[i] + more
            spare = spare - more
    return np.array([most] + holding)


def ragged(key, amount, total, bound, skew):
    if amount == 2:
        one = jax.random.randint(key, (), max(1, total - bound), min(bound, total - 1) + 1)
        return jnp.stack([one, total - one])
    lengths = jnp.asarray(profile(amount, total, bound, skew), jnp.int32)
    couples = (amount - 1) // 2
    donor, receiver = lengths[1:1 + 2 * couples:2], lengths[2:2 + 2 * couples:2]
    room = jnp.minimum(donor - 1, bound - receiver)
    passed = jax.random.randint(jax.random.fold_in(key, 1), (couples,), 0, 1 << 20) % (room + 1)
    lengths = lengths.at[1:1 + 2 * couples:2].set(donor - passed).at[2:2 + 2 * couples:2].set(receiver + passed)
    return lengths[jax.random.permutation(jax.random.fold_in(key, 2), amount)]


def setup_inputs(seed: int = 0) -> dict:
    streams_of = jax.random.split(jax.random.key(seed), 5)
    return {
        "weights": draw_weights(jax.random.fold_in(streams_of[4], 71), 0),
        "left_bits": place_ends(jax.random.randint(streams_of[1], (EXPERTS, D), 0, 2), jax.random.fold_in(streams_of[1], 1), 0, 1).astype(jnp.int32),
        "right_bits": place_ends(jax.random.randint(streams_of[2], (EXPERTS, FF), 0, 2), jax.random.fold_in(streams_of[2], 1), 0, 1).astype(jnp.int32),
        "groups": jax.vmap(lambda own: jnp.searchsorted(jnp.cumsum(ragged(own, GROUPS, FF, GROUP_MOST, 1)), jnp.arange(FF), side="right"))(jax.random.split(streams_of[3], EXPERTS)).reshape((EXPERTS, FF)).astype(jnp.int32),
    }


def sylvester(order):
    row_index = jnp.arange(order, dtype=jnp.int32)[:, None]
    col_index = jnp.arange(order, dtype=jnp.int32)[None, :]
    common = jnp.bitwise_and(row_index, col_index)
    parity = jnp.zeros((order, order), jnp.int32)
    for bit_pos in range(order.bit_length() - 1):
        parity = parity + jnp.bitwise_and(jnp.right_shift(common, bit_pos), 1)
    return (1 - 2 * jnp.bitwise_and(parity, 1)).astype(jnp.float32)

def cosine_block(order):
    first = jnp.arange(order, dtype=jnp.float32)[:, None]
    second = jnp.arange(order, dtype=jnp.float32)[None, :]
    table = math.sqrt(2.0 / order) * jnp.cos(math.pi * (2.0 * second + 1.0) * first / (2.0 * order))
    return jnp.where(first == 0.0, table * math.sqrt(0.5), table)

def coset_error(values):
    nearest = jnp.floor(values + 0.5)
    offset = values - nearest
    squares = lax.optimization_barrier(jnp.sum(offset * offset, axis=-1))
    largest = lax.optimization_barrier(jnp.max(jnp.abs(offset), axis=-1))
    parity = jnp.mod(lax.optimization_barrier(jnp.sum(nearest, axis=-1)), 2.0)
    return jnp.where(parity > 0.5, squares + 1.0 - 2.0 * largest, squares)

def lattice_error(values):
    octets = values.reshape(values.shape[:-1] + (values.shape[-1] // 8, 8))
    return jnp.minimum(coset_error(octets), coset_error(octets - 0.5))

def reference(weights, left_bits, right_bits, groups):
    column_hadamard = sylvester(FF // OUTER)
    outer_hadamard = sylvester(OUTER)
    row_hadamard = sylvester(HB)
    block_matrix = cosine_block(BLOCKS).astype(jnp.bfloat16).astype(jnp.float32)
    group_ids = jnp.arange(GROUPS, dtype=jnp.int32)
    row_weight = (1.0 + 4.0 * (jnp.arange(D, dtype=jnp.float32) + 0.5) / D) / 3.0
    high = lax.Precision.HIGHEST

    def one_expert(operands):
        weight, left, right, group = operands
        left_sign = (2 * left - 1).astype(jnp.float32)
        right_sign = (2 * right - 1).astype(jnp.float32)
        signed = (weight.astype(jnp.float32) * left_sign[:, None] * right_sign[None, :]).astype(jnp.bfloat16)
        shaped = signed.astype(jnp.float32).reshape(D, OUTER, FF // OUTER)
        inner = jnp.einsum('dpq,qs->dps', shaped, column_hadamard, precision=high)
        outer = jnp.einsum('dps,pt->dts', inner, outer_hadamard, precision=high)
        columns = (outer.reshape(D, FF) / math.sqrt(FF)).astype(jnp.bfloat16)
        blocked = columns.astype(jnp.float32).reshape(BLOCKS, HB, FF)
        mixed_rows = jnp.einsum('ij,jbf->ibf', block_matrix, blocked, precision=high)
        rotated = jnp.einsum('ibf,bk->ikf', mixed_rows, row_hadamard, precision=high) / math.sqrt(HB)
        rotated = rotated.reshape(D, FF)
        column_peak = lax.optimization_barrier(jnp.max(jnp.abs(rotated), axis=0))
        in_group = group[None, :] == group_ids[:, None]
        group_peak = jnp.maximum(lax.optimization_barrier(jnp.max(jnp.where(in_group, column_peak[None, :], 0.0), axis=1)), 1.0)
        column_scale = lax.optimization_barrier(jnp.sum(jnp.where(in_group, (2.0 / group_peak)[:, None], 0.0), axis=0))
        values = rotated * column_scale[None, :]
        block_errors = lattice_error(values)
        mean_error = jnp.sum(block_errors * row_weight[:, None]) / (D * FF // 8)
        return (values.astype(jnp.bfloat16), block_errors, group_peak / 2.0, mean_error)
    scaled, block_error, scales, expert_error = lax.map(one_expert, (weights, left_bits, right_bits, groups))
    total_error = jnp.mean(expert_error)
    return (scaled, block_error, scales, expert_error, total_error)
```

```python
import functools
import math

import jax
import jax.numpy as jnp
import ml_dtypes
import numpy as np
from jax import lax
from jax.experimental import pallas as pl
from jax.experimental.pallas import tpu as pltpu
from jax.sharding import PartitionSpec as P

D = 7168
FF = 2048
HB = 128
GROUPS = 16
BLOCKS = 56
ROWS = 8
PEERS = 16
MINE = BLOCKS // ROWS
LANES = 128
MESH = pl.DeviceIdType.MESH
F32 = jnp.float32
BF16 = jnp.bfloat16


def cosine_table():
    first = np.arange(BLOCKS, dtype=np.float64)[:, None]
    second = np.arange(BLOCKS, dtype=np.float64)[None, :]
    table = math.sqrt(2.0 / BLOCKS) * np.cos(math.pi * (2.0 * second + 1.0) * first / (2.0 * BLOCKS))
    table[0] *= math.sqrt(0.5)
    padded = np.zeros((64, LANES), np.float32)
    padded[:BLOCKS, :BLOCKS] = table
    return padded.astype(ml_dtypes.bfloat16)


def iota(shape, dim):
    return lax.broadcasted_iota(jnp.int32, shape, dim)


def sign_of(common, bits):
    parity = common
    shift = bits // 2
    while shift:
        parity = jnp.bitwise_xor(parity, jnp.right_shift(parity, shift))
        shift //= 2
    return (1 - 2 * jnp.bitwise_and(parity, 1)).astype(F32)


def butterfly(parts):
    parts = list(parts)
    step = 1
    while step < len(parts):
        for low in range(len(parts)):
            if not low & step:
                a, b = parts[low], parts[low + step]
                parts[low], parts[low + step] = a + b, a - b
        step *= 2
    return parts


def odd(count):
    return count - 2.0 * jnp.floor(count * 0.5) > 0.5


def lattice(values):
    first = None
    for value in values:
        whole = jnp.floor(value)
        g = jnp.abs((value - whole) - 0.5)
        near = jnp.floor(value + 0.5)
        now = (g, g * g, g, g, whole, near)
        if first is None:
            first = now
        else:
            first = (
                first[0] + now[0],
                first[1] + now[1],
                jnp.maximum(first[2], g),
                jnp.minimum(first[3], g),
                first[4] + whole,
                first[5] + near,
            )
    total, squares, most, least, halves, wholes = first
    shifted = jnp.where(odd(halves), squares + 1.0 - 2.0 * most, squares)
    plain = 2.0 - total + squares
    plain = jnp.where(odd(wholes), plain + 2.0 * least, plain)
    return jnp.minimum(plain, shifted)


def kernel(
    w_ref, lb_ref, rb_ref, g_ref, cos_ref,
    scaled_ref, err_ref, scale_ref, expert_ref, total_ref,
    wv, had, perm, mix, right, left, signed, inner, sb1, rb1, mid, rot, rb2, ybuf,
    gperm, cs_nat, cs_perm, pk_s, pk_r, e_s, e_r, t_s, t_r,
    w_sem, s1_send, s1_recv, s2_send, s2_recv, pk_send, pk_recv, e_send, e_recv, t_send, t_recv,
):
    me = lax.axis_index("row")
    ex = lax.axis_index("expert")
    row_peer = [lax.rem(me + k, ROWS) for k in range(1, ROWS)]
    ex_peer = [lax.rem(ex + k, PEERS) for k in range(1, PEERS)]

    loads = []
    for i in range(MINE):
        loads.append(pltpu.make_async_copy(w_ref.at[0, pl.ds(i * HB, HB)], wv.at[pl.ds(i * HB, HB)], w_sem.at[i]))
        loads[-1].start()
    barrier = pltpu.get_barrier_semaphore()
    for p in row_peer:
        pl.semaphore_signal(barrier, inc=1, device_id={"row": p}, device_id_type=MESH)
    for p in ex_peer:
        pl.semaphore_signal(barrier, inc=1, device_id={"expert": p}, device_id_type=MESH)

    had[...] = sign_of(jnp.bitwise_and(iota((256, 256), 0), iota((256, 256), 1)), 8).astype(BF16)
    right[...] = jnp.broadcast_to((2 * rb_ref[...] - 1).astype(F32), (16, FF)).astype(BF16)
    for i in range(MINE):
        signs = (2 * lb_ref[:, i * HB:(i + 1) * HB] - 1).astype(F32)
        left[i] = jnp.broadcast_to(signs, (HB, LANES)).T.astype(BF16)

    for load in loads:
        load.wait()

    def column_block(i, carry):
        first = pl.multiple_of(i * HB, HB)
        lefts = jnp.concatenate([left[i], left[i]], axis=1)
        for p in range(8):
            x = wv[pl.ds(first, HB), p * 256:(p + 1) * 256]
            signed[p * HB:(p + 1) * HB, :] = x * lefts * right[0:1, p * 256:(p + 1) * 256]
        inner[...] = jnp.dot(signed[...], had[...], preferred_element_type=F32)
        for u in range(2):
            for r in range(HB // 16):
                parts = [inner[p * HB + r * 16:p * HB + (r + 1) * 16, u * LANES:(u + 1) * LANES] for p in range(8)]
                for t, part in enumerate(butterfly(parts)):
                    sb1[t // 4, (t % 4) * 2 + u, i, r * 16:(r + 1) * 16, :] = (part * (1.0 / math.sqrt(FF))).astype(BF16)
        return carry

    lax.fori_loop(0, MINE, column_block, 0)
    pl.semaphore_wait(barrier, ROWS + PEERS - 2)

    for h in range(2):
        for p in row_peer:
            pltpu.make_async_remote_copy(
                sb1.at[h, p], rb1.at[h, me], s1_send.at[h], s1_recv.at[h], device_id={"row": p}, device_id_type=MESH
            ).start()
    for h in range(2):
        rb1[h, me] = sb1[h, me]

    pick_a = (jnp.right_shift(iota((896, 64), 0), 4) == iota((896, 64), 1)).astype(F32).astype(BF16)
    spread = jnp.dot(pick_a, cos_ref[...], preferred_element_type=F32).astype(BF16)
    pick_j = (jnp.right_shift(iota((LANES, 896), 1), 4) == iota((LANES, 896), 0)).astype(F32).astype(BF16)
    mix[...] = jnp.dot(spread, pick_j, preferred_element_type=F32).astype(BF16)
    small = sign_of(
        jnp.bitwise_and(jnp.bitwise_and(iota((16, 896), 0), iota((16, 896), 1)), 15), 4
    ).astype(BF16)

    def sign_mix(a, carry):
        at = pl.ds(pl.multiple_of(a * 16, 16), 16)
        mix[at, :] = mix[at, :] * small
        return carry

    lax.fori_loop(0, BLOCKS, sign_mix, 0)
    for s in range(8):
        perm[:, s * LANES:(s + 1) * LANES] = (
            iota((1024, LANES), 0) == 8 * iota((1024, LANES), 1) + s
        ).astype(F32).astype(BF16)
    which = iota((16, 1024), 0)
    ids = jnp.zeros((16, 1024), F32)
    for h in range(2):
        ids = jnp.where(which == h, g_ref[:, h * 1024:(h + 1) * 1024].astype(F32), ids)
        own = g_ref[:, pl.ds(pl.multiple_of(h * 1024 + me * LANES, LANES), LANES)].astype(F32)
        ids = jnp.where(which == 2 + h, jnp.concatenate([own] * 8, axis=1), ids)
    gperm[...] = jnp.dot(ids.astype(BF16), perm[...], preferred_element_type=F32)

    def rotate_rows(h):
        pltpu.make_async_copy(rb1.at[h, pl.ds(0, ROWS - 1)], rb1.at[h, pl.ds(0, ROWS - 1)], s1_recv.at[h]).wait()

        def mix_blocks(q, carry):
            parts = []
            for half in range(2):
                at = pl.ds(pl.multiple_of(q * 32 + half * 16, 16), 16)
                parts.append(rb1[h, :, :, at, :].reshape(896, LANES))
            out = jnp.dot(mix[...], jnp.concatenate(parts, axis=1), preferred_element_type=F32)
            mid[2 * q] = out[:, :LANES]
            mid[2 * q + 1] = out[:, LANES:]
            return carry

        lax.fori_loop(0, 4, mix_blocks, 0)

        def turn(a, peak):
            at = pl.ds(pl.multiple_of(a * 16, 16), 16)
            parts = butterfly([mid[q, at, :] for q in range(8)])
            for q, part in enumerate(parts):
                part = part * (1.0 / math.sqrt(HB))
                peak = jnp.maximum(peak, jnp.abs(part))
                rot[h, a // MINE, lax.rem(a, MINE), q * 16:(q + 1) * 16, :] = part.astype(BF16)
            return peak

        peak = lax.fori_loop(0, BLOCKS, turn, jnp.zeros((16, LANES), F32))
        rb2[h, me] = rot[h, me]
        return jnp.max(peak, axis=0, keepdims=True)

    def send_rows(h, blocks):
        for i in blocks:
            for p in row_peer:
                pltpu.make_async_remote_copy(
                    rot.at[h, p, i], rb2.at[h, me, i], s2_send.at[h], s2_recv.at[h, i], device_id={"row": p}, device_id_type=MESH
                ).start()

    def exchange(slots, own, source, send, recv, here, peers, axis):
        slots[here] = own
        source[...] = own
        for p in peers:
            pltpu.make_async_remote_copy(
                source, slots.at[here], send, recv, device_id={axis: p}, device_id_type=MESH
            ).start()

    def arrived(slots, recv, count):
        pltpu.make_async_copy(slots.at[pl.ds(0, count)], slots.at[pl.ds(0, count)], recv).wait()

    col_peak = [rotate_rows(0)]
    send_rows(0, range(0, 2))
    col_peak.append(rotate_rows(1))

    group_id = iota((GROUPS, LANES), 0)
    most = jnp.zeros((GROUPS, LANES), F32)
    for h in range(2):
        own = g_ref[:, pl.ds(pl.multiple_of(h * 1024 + me * LANES, LANES), LANES)]
        most = jnp.maximum(most, jnp.where(group_id == own, col_peak[h], 0.0))
    most = jnp.broadcast_to(jnp.max(most, axis=1, keepdims=True), (GROUPS, LANES))
    exchange(pk_r, most, pk_s, pk_send, pk_recv, me, row_peer, "row")
    send_rows(0, range(2, MINE))

    arrived(pk_r, pk_recv, ROWS - 1)
    group_peak = jnp.ones((GROUPS, LANES), F32)
    for k in range(ROWS):
        group_peak = jnp.maximum(group_peak, pk_r[k])
    scale_row = jnp.sum(
        jnp.where(group_id == iota((GROUPS, LANES), 1), group_peak * 0.5, 0.0), axis=0, keepdims=True
    )
    scale_ref[...] = scale_row[:, :GROUPS]
    inverse = 2.0 / group_peak
    for m in range(16):
        ids = g_ref[:, m * LANES:(m + 1) * LANES]
        cs_nat[m:m + 1, :] = jnp.sum(jnp.where(group_id == ids, inverse, 0.0), axis=0, keepdims=True)
    for k in range(4):
        for s in range(8):
            ids = gperm[k:k + 1, s * LANES:(s + 1) * LANES]
            cs_perm[k, s:s + 1, :] = jnp.sum(
                jnp.where(group_id.astype(F32) == ids, inverse, 0.0), axis=0, keepdims=True
            )

    def own_errors(n, total):
        parts = []
        for h in range(2):
            blocks = []
            for k in range(8):
                a = n * 8 + k
                blocks.append(rot[h, a // MINE, lax.rem(a, MINE)])
            parts.append(jnp.concatenate(blocks, axis=1))
        ybuf[...] = jnp.dot(jnp.concatenate(parts, axis=0), perm[...], preferred_element_type=F32)
        block = n * 8 + jnp.right_shift(iota((8, LANES), 1), 4)
        for h in range(2):
            scales = [cs_perm[2 + h, s:s + 1, :] for s in range(8)]

            def rows(r, total):
                at = pl.ds(pl.multiple_of(h * HB + r * 8, 8), 8)
                errors = lattice([ybuf[at, s * LANES:(s + 1) * LANES] * scales[s] for s in range(8)])
                row = (block * HB + r * 8 + iota((8, LANES), 0)).astype(F32)
                return total + errors * ((1.0 + 4.0 * (row + 0.5) / D) / 3.0)

            total = lax.fori_loop(0, HB // 8, rows, total, unroll=4)
        return total

    error = lax.fori_loop(0, MINE, own_errors, jnp.zeros((8, LANES), F32))
    exchange(e_r, error, e_s, e_send, e_recv, me, row_peer, "row")
    send_rows(1, range(0, 2))

    def finish(h, i):
        pltpu.make_async_copy(
            rb2.at[h, pl.ds(0, ROWS - 1), i], rb2.at[h, pl.ds(0, ROWS - 1), i], s2_recv.at[h, i]
        ).wait()
        first = pl.multiple_of(i * HB, HB)
        blocks = [rb2[h, k, i] for k in range(ROWS)]
        ybuf[:HB, :] = jnp.dot(jnp.concatenate(blocks, axis=1), perm[...], preferred_element_type=F32)
        for k in range(ROWS):
            m = h * 8 + k
            scaled_ref[0, pl.ds(first, HB), m * LANES:(m + 1) * LANES] = (
                blocks[k].astype(F32) * cs_nat[m:m + 1, :]
            ).astype(BF16)
        scales = [cs_perm[h, s:s + 1, :] for s in range(8)]

        def rows(r, carry):
            at = pl.ds(pl.multiple_of(r * 8, 8), 8)
            errors = lattice([ybuf[at, s * LANES:(s + 1) * LANES] * scales[s] for s in range(8)])
            err_ref[0, pl.ds(pl.multiple_of(first + r * 8, 8), 8), h * LANES:(h + 1) * LANES] = errors
            return carry

        lax.fori_loop(0, HB // 8, rows, 0, unroll=4)

    def finish_many(h, start, stop):
        def step(i, carry):
            finish(h, i)
            return carry

        lax.fori_loop(start, stop, step, 0)

    finish_many(0, 0, 3)
    arrived(e_r, e_recv, ROWS - 1)
    error = e_r[0]
    for k in range(1, ROWS):
        error = error + e_r[k]
    error = jnp.sum(jnp.sum(error, axis=1, keepdims=True), axis=0, keepdims=True) * (1.0 / (D * FF // 8))
    expert_ref[...] = error
    exchange(t_r, jnp.broadcast_to(error, (8, LANES)), t_s, t_send, t_recv, ex, ex_peer, "expert")
    send_rows(1, range(2, MINE))
    finish_many(0, 3, MINE)
    arrived(t_r, t_recv, PEERS - 1)
    total = t_r[0]
    for k in range(1, PEERS):
        total = total + t_r[k]
    total_ref[...] = total[:1, :1] * (1.0 / PEERS)
    finish_many(1, 0, MINE)

    for h in range(2):
        pltpu.make_async_copy(sb1.at[h, pl.ds(0, ROWS - 1)], sb1.at[h, pl.ds(0, ROWS - 1)], s1_send.at[h]).wait()
        pltpu.make_async_copy(rot.at[h, pl.ds(0, ROWS - 1)], rot.at[h, pl.ds(0, ROWS - 1)], s2_send.at[h]).wait()
    arrived(pk_r, pk_send, ROWS - 1)
    arrived(e_r, e_send, ROWS - 1)
    arrived(t_r, t_send, PEERS - 1)


def body(weights, left_bits, right_bits, groups):
    vmem = pl.BlockSpec(memory_space=pltpu.VMEM)
    any_space = pl.BlockSpec(memory_space=pl.ANY)
    scaled, errors, scales, expert_error, total_error = pl.pallas_call(
        kernel,
        out_shape=(
            jax.ShapeDtypeStruct((1, MINE * HB, FF), BF16),
            jax.ShapeDtypeStruct((1, MINE * HB, FF // 8), F32),
            jax.ShapeDtypeStruct((1, GROUPS), F32),
            jax.ShapeDtypeStruct((1, 1), F32),
            jax.ShapeDtypeStruct((1, 1), F32),
        ),
        in_specs=[any_space, vmem, vmem, vmem, vmem],
        out_specs=(vmem,) * 5,
        scratch_shapes=[
            pltpu.VMEM((MINE * HB, FF), BF16),
            pltpu.VMEM((256, 256), BF16),
            pltpu.VMEM((1024, 1024), BF16),
            pltpu.VMEM((896, 896), BF16),
            pltpu.VMEM((16, FF), BF16),
            pltpu.VMEM((MINE, HB, LANES), BF16),
            pltpu.VMEM((8 * HB, 256), BF16),
            pltpu.VMEM((8 * HB, 256), F32),
            pltpu.VMEM((2, ROWS, MINE, HB, LANES), BF16),
            pltpu.VMEM((2, ROWS, MINE, HB, LANES), BF16),
            pltpu.VMEM((8, 896, LANES), F32),
            pltpu.VMEM((2, ROWS, MINE, HB, LANES), BF16),
            pltpu.VMEM((2, ROWS, MINE, HB, LANES), BF16),
            pltpu.VMEM((2 * HB, 1024), F32),
            pltpu.VMEM((16, 1024), F32),
            pltpu.VMEM((16, LANES), F32),
            pltpu.VMEM((4, 8, LANES), F32),
            pltpu.VMEM((GROUPS, LANES), F32),
            pltpu.VMEM((ROWS, GROUPS, LANES), F32),
            pltpu.VMEM((8, LANES), F32),
            pltpu.VMEM((ROWS, 8, LANES), F32),
            pltpu.VMEM((8, LANES), F32),
            pltpu.VMEM((PEERS, 8, LANES), F32),
            pltpu.SemaphoreType.DMA((MINE,)),
            pltpu.SemaphoreType.DMA((2,)),
            pltpu.SemaphoreType.DMA((2,)),
            pltpu.SemaphoreType.DMA((2,)),
            pltpu.SemaphoreType.DMA((2, MINE)),
            pltpu.SemaphoreType.DMA,
            pltpu.SemaphoreType.DMA,
            pltpu.SemaphoreType.DMA,
            pltpu.SemaphoreType.DMA,
            pltpu.SemaphoreType.DMA,
            pltpu.SemaphoreType.DMA,
        ],
        compiler_params=pltpu.CompilerParams(
            collective_id=0, has_side_effects=True, vmem_limit_bytes=60 * 2**20
        ),
        name="rotate",
    )(weights, left_bits, right_bits, groups, jnp.asarray(cosine_table()))
    return scaled, errors, scales, expert_error.reshape(1), total_error.reshape(())


def solution(mesh):
    placed = (P("expert", "row", None), P("expert", "row"), P("expert", None), P("expert", None))
    return jax.shard_map(
        body,
        mesh=mesh,
        in_specs=placed,
        out_specs=(
            P("expert", "row", None),
            P("expert", "row", None),
            P("expert", None),
            P("expert"),
            P(),
        ),
        check_vma=False,
    )
```

```python
import math

import jax
import jax.numpy as jnp
import ml_dtypes
import numpy as np
from jax import lax
from jax.experimental import pallas as pl
from jax.experimental.pallas import tpu as pltpu
from jax.sharding import PartitionSpec as P

D = 7168
FF = 2048
HB = 128
GROUPS = 16
BLOCKS = 56
ROWS = 8
PEERS = 16
MINE = BLOCKS // ROWS
LANES = 128
MESH = pl.DeviceIdType.MESH
TOTAL_ORDER = (8, 1, 2, 4)
FIRST = 2
MIDDLE = 4
VMEM_LIMIT = 56 * 2**20
F32 = jnp.float32
BF16 = jnp.bfloat16


def cosine_table():
    first = np.arange(BLOCKS, dtype=np.float64)[:, None]
    second = np.arange(BLOCKS, dtype=np.float64)[None, :]
    table = math.sqrt(2.0 / BLOCKS) * np.cos(math.pi * (2.0 * second + 1.0) * first / (2.0 * BLOCKS))
    table[0] *= math.sqrt(0.5)
    padded = np.zeros((64, LANES), np.float32)
    padded[:BLOCKS, :BLOCKS] = table
    return padded.astype(ml_dtypes.bfloat16)


def iota(shape, dim):
    return lax.broadcasted_iota(jnp.int32, shape, dim)


def sign_of(common, bits):
    parity = common
    shift = bits // 2
    while shift:
        parity = jnp.bitwise_xor(parity, jnp.right_shift(parity, shift))
        shift //= 2
    return (1 - 2 * jnp.bitwise_and(parity, 1)).astype(F32)


def butterfly(parts):
    parts = list(parts)
    step = 1
    while step < len(parts):
        for low in range(len(parts)):
            if not low & step:
                a, b = parts[low], parts[low + step]
                parts[low], parts[low + step] = a + b, a - b
        step *= 2
    return parts


def odd(count):
    return count - 2.0 * jnp.floor(count * 0.5) > 0.5


def lattice(values):
    first = None
    for value in values:
        whole = jnp.floor(value)
        g = jnp.abs((value - whole) - 0.5)
        near = jnp.floor(value + 0.5)
        now = (g, g * g, g, g, whole, near)
        if first is None:
            first = now
        else:
            first = (
                first[0] + now[0],
                first[1] + now[1],
                jnp.maximum(first[2], g),
                jnp.minimum(first[3], g),
                first[4] + whole,
                first[5] + near,
            )
    total, squares, most, least, halves, wholes = first
    shifted = jnp.where(odd(halves), squares + 1.0 - 2.0 * most, squares)
    plain = 2.0 - total + squares
    plain = jnp.where(odd(wholes), plain + 2.0 * least, plain)
    return jnp.minimum(plain, shifted)


def push(src, dst, send, recv, device):
    pltpu.make_async_remote_copy(src, dst, send, recv, device_id=device, device_id_type=MESH).start()


def arrived(ref, sem):
    pltpu.make_async_copy(ref, ref, sem).wait()


def finish_block(blocks, perm, ybuf, natural, permuted, put_scaled, put_errors):
    ybuf[:HB, :] = jnp.dot(jnp.concatenate(blocks, axis=1), perm[...], preferred_element_type=F32)
    for k in range(ROWS):
        put_scaled(k, (blocks[k].astype(F32) * natural[k]).astype(BF16))

    def rows(r, carry):
        at = pl.ds(pl.multiple_of(r * 8, 8), 8)
        put_errors(r, lattice([ybuf[at, s * LANES:(s + 1) * LANES] * permuted[s] for s in range(8)]))
        return carry

    lax.fori_loop(0, HB // 8, rows, 0, unroll=4)


def rotate_kernel(
    w_ref, lb_ref, rb_ref, g_ref, cos_ref,
    scaled_ref, err_ref, small_ref, last_ref, perm, cs_nat, cs_perm,
    wv, lb, rb, gv, cosv, had, mix, right, left, signed, inner, sb1, rb1, mid, rot, rb2, ybuf,
    gperm, pk_s, pk_r, e_s, e_r, t_s, t_r,
    w_sem, in_sem, s1_send, s1_recv, s2_send, s2_recv, pk_send, pk_recv, e_send, e_recv, t_send, t_recv,
):
    me = lax.axis_index("row")
    ex = lax.axis_index("expert")
    row_peer = [lax.rem(me + k, ROWS) for k in range(1, ROWS)]
    ex_peer = [jnp.bitwise_xor(ex, bit) for bit in TOTAL_ORDER]

    small_loads = [
        pltpu.make_async_copy(src, dst, in_sem.at[n])
        for n, (src, dst) in enumerate(((lb_ref, lb), (rb_ref, rb), (g_ref, gv), (cos_ref, cosv)))
    ]
    loads = [
        pltpu.make_async_copy(w_ref.at[0, pl.ds(i * HB, HB)], wv.at[pl.ds(i * HB, HB)], w_sem.at[i])
        for i in range(MINE)
    ]
    for load in small_loads[:2] + loads[:1]:
        load.start()
    barrier = pltpu.get_barrier_semaphore()
    for p in row_peer:
        pl.semaphore_signal(barrier, inc=1, device_id={"row": p}, device_id_type=MESH)
    for p in ex_peer:
        pl.semaphore_signal(barrier, inc=1, device_id={"expert": p}, device_id_type=MESH)
    for load in loads[1:] + small_loads[2:]:
        load.start()

    had[...] = sign_of(jnp.bitwise_and(iota((256, 256), 0), iota((256, 256), 1)), 8).astype(BF16)
    small_loads[0].wait()
    small_loads[1].wait()
    right[...] = jnp.broadcast_to((2 * rb[...] - 1).astype(F32), (16, FF)).astype(BF16)

    def left_signs(i, carry):
        signs = (2 * lb[:, pl.ds(pl.multiple_of(i * HB, HB), HB)] - 1).astype(F32)
        left[i] = jnp.broadcast_to(signs, (HB, LANES)).T.astype(BF16)
        return carry

    left_signs(0, 0)

    def column_block(i):
        first = pl.multiple_of(i * HB, HB)
        lefts = jnp.concatenate([left[i], left[i]], axis=1)
        for p in range(8):
            x = wv[pl.ds(first, HB), p * 256:(p + 1) * 256]
            signed[p * HB:(p + 1) * HB, :] = x * lefts * right[0:1, p * 256:(p + 1) * 256]
        inner[...] = jnp.dot(signed[...], had[...], preferred_element_type=F32)
        for u in range(2):
            for r in range(HB // 16):
                parts = [inner[p * HB + r * 16:p * HB + (r + 1) * 16, u * LANES:(u + 1) * LANES] for p in range(8)]
                for t, part in enumerate(butterfly(parts)):
                    sb1[t // 4, (t % 4) * 2 + u, i, r * 16:(r + 1) * 16, :] = (part * (1.0 / math.sqrt(FF))).astype(BF16)

    def send_columns(i):
        for p in row_peer:
            push(sb1.at[0, p, i], rb1.at[0, me, i], s1_send.at[0], s1_recv.at[0], {"row": p})

    loads[0].wait()
    column_block(0)
    pl.semaphore_wait(barrier, ROWS - 1 + len(TOTAL_ORDER))
    send_columns(0)
    lax.fori_loop(1, MINE, left_signs, 0)

    def column_step(i, carry):
        pltpu.make_async_copy(w_ref.at[0, pl.ds(0, HB)], wv.at[pl.ds(0, HB)], w_sem.at[i]).wait()
        column_block(i)
        send_columns(i)
        return carry

    lax.fori_loop(1, MINE, column_step, 0)
    for p in row_peer:
        push(sb1.at[1, p], rb1.at[1, me], s1_send.at[1], s1_recv.at[1], {"row": p})
    for h in range(2):
        rb1[h, me] = sb1[h, me]

    small_loads[2].wait()
    small_loads[3].wait()
    pick_a = (jnp.right_shift(iota((896, 64), 0), 4) == iota((896, 64), 1)).astype(F32).astype(BF16)
    spread = jnp.dot(pick_a, cosv[...], preferred_element_type=F32).astype(BF16)
    pick_j = (jnp.right_shift(iota((LANES, 896), 1), 4) == iota((LANES, 896), 0)).astype(F32).astype(BF16)
    mix[...] = jnp.dot(spread, pick_j, preferred_element_type=F32).astype(BF16)
    small = sign_of(
        jnp.bitwise_and(jnp.bitwise_and(iota((16, 896), 0), iota((16, 896), 1)), 15), 4
    ).astype(BF16)

    def sign_mix(a, carry):
        at = pl.ds(pl.multiple_of(a * 16, 16), 16)
        mix[at, :] = mix[at, :] * small
        return carry

    lax.fori_loop(0, BLOCKS, sign_mix, 0)
    for s in range(8):
        perm[:, s * LANES:(s + 1) * LANES] = (
            iota((1024, LANES), 0) == 8 * iota((1024, LANES), 1) + s
        ).astype(F32).astype(BF16)
    which = iota((16, 1024), 0)
    ids = jnp.zeros((16, 1024), F32)
    for h in range(2):
        ids = jnp.where(which == h, gv[:, h * 1024:(h + 1) * 1024].astype(F32), ids)
        own = gv[:, pl.ds(pl.multiple_of(h * 1024 + me * LANES, LANES), LANES)].astype(F32)
        ids = jnp.where(which == 2 + h, jnp.concatenate([own] * 8, axis=1), ids)
    gperm[...] = jnp.dot(ids.astype(BF16), perm[...], preferred_element_type=F32)

    def rotate_rows(h):
        arrived(rb1.at[h, pl.ds(0, ROWS - 1)], s1_recv.at[h])

        def mix_blocks(q, carry):
            parts = []
            for half in range(2):
                at = pl.ds(pl.multiple_of(q * 32 + half * 16, 16), 16)
                parts.append(rb1[h, :, :, at, :].reshape(896, LANES))
            out = jnp.dot(mix[...], jnp.concatenate(parts, axis=1), preferred_element_type=F32)
            mid[2 * q] = out[:, :LANES]
            mid[2 * q + 1] = out[:, LANES:]
            return carry

        lax.fori_loop(0, 4, mix_blocks, 0)

        def turn(a, peak):
            at = pl.ds(pl.multiple_of(a * 16, 16), 16)
            parts = butterfly([mid[q, at, :] for q in range(8)])
            for q, part in enumerate(parts):
                part = part * (1.0 / math.sqrt(HB))
                peak = jnp.maximum(peak, jnp.abs(part))
                rot[h, a // MINE, lax.rem(a, MINE), q * 16:(q + 1) * 16, :] = part.astype(BF16)
            return peak

        peak = lax.fori_loop(0, BLOCKS, turn, jnp.zeros((16, LANES), F32))
        rb2[h, me] = rot[h, me]
        return jnp.max(peak, axis=0, keepdims=True)

    def send_rows(h, blocks):
        for i in blocks:
            for p in row_peer:
                push(rot.at[h, p, i], rb2.at[h, me, i], s2_send.at[h], s2_recv.at[h, i], {"row": p})

    def to_row(slots, own, source, send, recv):
        slots[me] = own
        source[...] = own
        for p in row_peer:
            push(source, slots.at[me], send, recv, {"row": p})

    col_peak = [rotate_rows(0)]
    send_rows(0, range(0, FIRST))
    col_peak.append(rotate_rows(1))

    group_id = iota((GROUPS, LANES), 0)
    most = jnp.zeros((GROUPS, LANES), F32)
    for h in range(2):
        own = gv[:, pl.ds(pl.multiple_of(h * 1024 + me * LANES, LANES), LANES)]
        most = jnp.maximum(most, jnp.where(group_id == own, col_peak[h], 0.0))
    most = jnp.broadcast_to(jnp.max(most, axis=1, keepdims=True), (GROUPS, LANES))
    to_row(pk_r, most, pk_s, pk_send, pk_recv)
    send_rows(0, range(FIRST, MINE))

    arrived(pk_r.at[pl.ds(0, ROWS - 1)], pk_recv)
    group_peak = jnp.ones((GROUPS, LANES), F32)
    for k in range(ROWS):
        group_peak = jnp.maximum(group_peak, pk_r[k])
    small_ref[0:1, :] = jnp.sum(
        jnp.where(group_id == iota((GROUPS, LANES), 1), group_peak * 0.5, 0.0), axis=0, keepdims=True
    )
    inverse = 2.0 / group_peak
    for m in range(16):
        ids = gv[:, m * LANES:(m + 1) * LANES]
        cs_nat[m:m + 1, :] = jnp.sum(jnp.where(group_id == ids, inverse, 0.0), axis=0, keepdims=True)
    for k in range(4):
        for s in range(8):
            ids = gperm[k:k + 1, s * LANES:(s + 1) * LANES]
            cs_perm[k, s:s + 1, :] = jnp.sum(
                jnp.where(group_id.astype(F32) == ids, inverse, 0.0), axis=0, keepdims=True
            )

    def own_errors(n, total):
        parts = []
        for h in range(2):
            blocks = []
            for k in range(8):
                a = n * 8 + k
                blocks.append(rot[h, a // MINE, lax.rem(a, MINE)])
            parts.append(jnp.concatenate(blocks, axis=1))
        ybuf[...] = jnp.dot(jnp.concatenate(parts, axis=0), perm[...], preferred_element_type=F32)
        block = n * 8 + jnp.right_shift(iota((8, LANES), 1), 4)
        for h in range(2):
            scales = [cs_perm[2 + h, s:s + 1, :] for s in range(8)]

            def rows(r, total):
                at = pl.ds(pl.multiple_of(h * HB + r * 8, 8), 8)
                errors = lattice([ybuf[at, s * LANES:(s + 1) * LANES] * scales[s] for s in range(8)])
                row = (block * HB + r * 8 + iota((8, LANES), 0)).astype(F32)
                return total + errors * ((1.0 + 4.0 * (row + 0.5) / D) / 3.0)

            total = lax.fori_loop(0, HB // 8, rows, total, unroll=4)
        return total

    error = lax.fori_loop(0, MIDDLE, own_errors, jnp.zeros((8, LANES), F32))
    send_rows(1, range(0, 1))
    error = lax.fori_loop(MIDDLE, MINE, own_errors, error)
    to_row(e_r, error, e_s, e_send, e_recv)
    send_rows(1, range(1, 2))

    def finish(h, start, stop):
        def step(i, carry):
            arrived(rb2.at[h, pl.ds(0, ROWS - 1), i], s2_recv.at[h, i])
            first = pl.multiple_of(i * HB, HB)

            def put_scaled(k, value):
                scaled_ref[0, pl.ds(first, HB), (h * 8 + k) * LANES:(h * 8 + k + 1) * LANES] = value

            def put_errors(r, value):
                err_ref[0, pl.ds(pl.multiple_of(first + r * 8, 8), 8), h * LANES:(h + 1) * LANES] = value

            finish_block(
                [rb2[h, k, i] for k in range(ROWS)], perm, ybuf,
                [cs_nat[h * 8 + k:h * 8 + k + 1, :] for k in range(ROWS)],
                [cs_perm[h, s:s + 1, :] for s in range(8)], put_scaled, put_errors,
            )
            return carry

        lax.fori_loop(start, stop, step, 0)

    finish(0, 0, 2)
    arrived(e_r.at[pl.ds(0, ROWS - 1)], e_recv)
    error = e_r[0]
    for k in range(1, ROWS):
        error = error + e_r[k]
    error = jnp.sum(jnp.sum(error, axis=1, keepdims=True), axis=0, keepdims=True) * (1.0 / (D * FF // 8))
    total = jnp.broadcast_to(error, (8, LANES))
    small_ref[1:2, :] = total[:1]
    done = 2
    for n, p in enumerate(ex_peer):
        t_s[n] = total
        push(t_s.at[n], t_r.at[n], t_send.at[n], t_recv.at[n], {"expert": p})
        send_rows(1, range(2 + n, 3 + n) if n < 3 else range(5, MINE))
        more = 2 if n == 0 else 1
        finish(0, done, done + more)
        done += more
        arrived(t_r.at[n], t_recv.at[n])
        total = total + t_r[n]
    small_ref[2:3, :] = total[:1] * (1.0 / PEERS)
    finish(1, 0, MINE - 1)
    arrived(rb2.at[1, pl.ds(0, ROWS - 1), MINE - 1], s2_recv.at[1, MINE - 1])
    for k in range(ROWS):
        last_ref[k] = rb2[1, k, MINE - 1]

    for h in range(2):
        arrived(sb1.at[h, pl.ds(0, ROWS - 1)], s1_send.at[h])
        arrived(rot.at[h, pl.ds(0, ROWS - 1)], s2_send.at[h])
    arrived(pk_r.at[pl.ds(0, ROWS - 1)], pk_send)
    arrived(e_r.at[pl.ds(0, ROWS - 1)], e_send)
    for n in range(len(TOTAL_ORDER)):
        arrived(t_s.at[n], t_send.at[n])


def finish_kernel(
    scaled, errors, small, last, perm, cs_nat, cs_perm,
    scaled_ref, err_ref, scale_ref, expert_ref, total_ref,
    ybuf, scaled_last, err_last, sems,
):
    edge = (MINE - 1) * HB
    half = FF // 2
    copies = [
        pltpu.make_async_copy(scaled.at[:, pl.ds(0, edge)], scaled_ref.at[:, pl.ds(0, edge)], sems.at[0]),
        pltpu.make_async_copy(
            scaled.at[:, pl.ds(edge, HB), pl.ds(0, half)], scaled_ref.at[:, pl.ds(edge, HB), pl.ds(0, half)], sems.at[1]
        ),
        pltpu.make_async_copy(errors.at[:, pl.ds(0, edge)], err_ref.at[:, pl.ds(0, edge)], sems.at[2]),
        pltpu.make_async_copy(
            errors.at[:, pl.ds(edge, HB), pl.ds(0, LANES)], err_ref.at[:, pl.ds(edge, HB), pl.ds(0, LANES)], sems.at[3]
        ),
    ]
    for copy in copies:
        copy.start()
    scale_ref[...] = small[0:1, :GROUPS]
    expert_ref[...] = small[1:2, :1]
    total_ref[...] = small[2:3, :1]

    def put_scaled(k, value):
        scaled_last[0, :, k * LANES:(k + 1) * LANES] = value

    def put_errors(r, value):
        err_last[0, pl.ds(pl.multiple_of(r * 8, 8), 8), :] = value

    finish_block(
        [last[k] for k in range(ROWS)], perm, ybuf,
        [cs_nat[8 + k:9 + k, :] for k in range(ROWS)],
        [cs_perm[1, s:s + 1, :] for s in range(8)], put_scaled, put_errors,
    )
    rest = [
        pltpu.make_async_copy(scaled_last, scaled_ref.at[:, pl.ds(edge, HB), pl.ds(half, half)], sems.at[4]),
        pltpu.make_async_copy(err_last, err_ref.at[:, pl.ds(edge, HB), pl.ds(LANES, LANES)], sems.at[5]),
    ]
    for copy in rest:
        copy.start()
    for copy in copies + rest:
        copy.wait()


def body(weights, left_bits, right_bits, groups):
    vmem = pl.BlockSpec(memory_space=pltpu.VMEM)
    hbm = pl.BlockSpec(memory_space=pltpu.HBM)
    rows = MINE * HB
    dma = pltpu.SemaphoreType.DMA
    arguments = [
        pltpu.with_memory_space_constraint(x, pltpu.HBM)
        for x in (weights, left_bits, right_bits, groups, jnp.asarray(cosine_table()))
    ]
    parts = pl.pallas_call(
        rotate_kernel,
        out_shape=(
            pltpu.VMEM((1, rows, FF), BF16),
            pltpu.VMEM((1, rows, FF // 8), F32),
            pltpu.VMEM((8, LANES), F32),
            pltpu.VMEM((ROWS, HB, LANES), BF16),
            pltpu.VMEM((1024, 1024), BF16),
            pltpu.VMEM((16, LANES), F32),
            pltpu.VMEM((4, 8, LANES), F32),
        ),
        in_specs=[hbm] * 5,
        out_specs=(vmem,) * 7,
        scratch_shapes=[
            pltpu.VMEM((rows, FF), BF16),
            pltpu.VMEM((1, rows), jnp.int32),
            pltpu.VMEM((1, FF), jnp.int32),
            pltpu.VMEM((1, FF), jnp.int32),
            pltpu.VMEM((64, LANES), BF16),
            pltpu.VMEM((256, 256), BF16),
            pltpu.VMEM((896, 896), BF16),
            pltpu.VMEM((16, FF), BF16),
            pltpu.VMEM((MINE, HB, LANES), BF16),
            pltpu.VMEM((8 * HB, 256), BF16),
            pltpu.VMEM((8 * HB, 256), F32),
            pltpu.VMEM((2, ROWS, MINE, HB, LANES), BF16),
            pltpu.VMEM((2, ROWS, MINE, HB, LANES), BF16),
            pltpu.VMEM((8, 896, LANES), F32),
            pltpu.VMEM((2, ROWS, MINE, HB, LANES), BF16),
            pltpu.VMEM((2, ROWS, MINE, HB, LANES), BF16),
            pltpu.VMEM((2 * HB, 1024), F32),
            pltpu.VMEM((16, 1024), F32),
            pltpu.VMEM((GROUPS, LANES), F32),
            pltpu.VMEM((ROWS, GROUPS, LANES), F32),
            pltpu.VMEM((8, LANES), F32),
            pltpu.VMEM((ROWS, 8, LANES), F32),
            pltpu.VMEM((len(TOTAL_ORDER), 8, LANES), F32),
            pltpu.VMEM((len(TOTAL_ORDER), 8, LANES), F32),
            dma((MINE,)),
            dma((4,)),
            dma((2,)),
            dma((2,)),
            dma((2,)),
            dma((2, MINE)),
            dma,
            dma,
            dma,
            dma,
            dma((len(TOTAL_ORDER),)),
            dma((len(TOTAL_ORDER),)),
        ],
        compiler_params=pltpu.CompilerParams(
            collective_id=0, has_side_effects=True, vmem_limit_bytes=VMEM_LIMIT
        ),
        name="rotate",
    )(*arguments)
    scaled, errors, scales, expert_error, total_error = pl.pallas_call(
        finish_kernel,
        out_shape=(
            jax.ShapeDtypeStruct((1, rows, FF), BF16),
            jax.ShapeDtypeStruct((1, rows, FF // 8), F32),
            jax.ShapeDtypeStruct((1, GROUPS), F32),
            jax.ShapeDtypeStruct((1, 1), F32),
            jax.ShapeDtypeStruct((1, 1), F32),
        ),
        in_specs=[vmem] * 7,
        out_specs=(hbm, hbm, vmem, vmem, vmem),
        scratch_shapes=[
            pltpu.VMEM((HB, 1024), F32),
            pltpu.VMEM((1, HB, FF // 2), BF16),
            pltpu.VMEM((1, HB, LANES), F32),
            dma((6,)),
        ],
        compiler_params=pltpu.CompilerParams(vmem_limit_bytes=8 * 2**20),
        name="finish",
    )(*parts)
    return scaled, errors, scales, expert_error.reshape(1), total_error.reshape(())


def solution(mesh):
    placed = (P("expert", "row", None), P("expert", "row"), P("expert", None), P("expert", None))
    return jax.shard_map(
        body,
        mesh=mesh,
        in_specs=placed,
        out_specs=(
            P("expert", "row", None),
            P("expert", "row", None),
            P("expert", None),
            P("expert"),
            P(),
        ),
        check_vma=False,
    )
```

```python
import math

import jax
import jax.numpy as jnp
import ml_dtypes
import numpy as np
from jax import lax
from jax.experimental import pallas as pl
from jax.experimental.pallas import tpu as pltpu
from jax.sharding import PartitionSpec as P

D = 7168
FF = 2048
HB = 128
GROUPS = 16
BLOCKS = 56
ROWS = 8
PEERS = 16
MINE = BLOCKS // ROWS
LANES = 128
MESH = pl.DeviceIdType.MESH
TOTAL_ORDER = ((8, 1), (1, 0), (2, 0), (4, 0))
FIRST = 3
MIDDLE = 4
VMEM_LIMIT = 56 * 2**20
F32 = jnp.float32
BF16 = jnp.bfloat16


def cosine_table():
    first = np.arange(BLOCKS, dtype=np.float64)[:, None]
    second = np.arange(BLOCKS, dtype=np.float64)[None, :]
    table = math.sqrt(2.0 / BLOCKS) * np.cos(math.pi * (2.0 * second + 1.0) * first / (2.0 * BLOCKS))
    table[0] *= math.sqrt(0.5)
    padded = np.zeros((64, LANES), np.float32)
    padded[:BLOCKS, :BLOCKS] = table
    return padded.astype(ml_dtypes.bfloat16)


def iota(shape, dim):
    return lax.broadcasted_iota(jnp.int32, shape, dim)


def sign_of(common, bits):
    parity = common
    shift = bits // 2
    while shift:
        parity = jnp.bitwise_xor(parity, jnp.right_shift(parity, shift))
        shift //= 2
    return (1 - 2 * jnp.bitwise_and(parity, 1)).astype(F32)


def butterfly(parts):
    parts = list(parts)
    step = 1
    while step < len(parts):
        for low in range(len(parts)):
            if not low & step:
                a, b = parts[low], parts[low + step]
                parts[low], parts[low + step] = a + b, a - b
        step *= 2
    return parts


def odd(count):
    return count - 2.0 * jnp.floor(count * 0.5) > 0.5


def lattice(values):
    first = None
    for value in values:
        whole = jnp.floor(value)
        g = jnp.abs((value - whole) - 0.5)
        near = jnp.floor(value + 0.5)
        now = (g, g * g, g, g, whole, near)
        if first is None:
            first = now
        else:
            first = (
                first[0] + now[0],
                first[1] + now[1],
                jnp.maximum(first[2], g),
                jnp.minimum(first[3], g),
                first[4] + whole,
                first[5] + near,
            )
    total, squares, most, least, halves, wholes = first
    shifted = jnp.where(odd(halves), squares + 1.0 - 2.0 * most, squares)
    plain = 2.0 - total + squares
    plain = jnp.where(odd(wholes), plain + 2.0 * least, plain)
    return jnp.minimum(plain, shifted)


def push(src, dst, send, recv, device):
    pltpu.make_async_remote_copy(src, dst, send, recv, device_id=device, device_id_type=MESH).start()


def arrived(ref, sem):
    pltpu.make_async_copy(ref, ref, sem).wait()


def finish_block(blocks, perm, ybuf, natural, permuted, put_scaled, put_errors):
    ybuf[:HB, :] = jnp.dot(jnp.concatenate(blocks, axis=1), perm[...], preferred_element_type=F32)
    for k in range(ROWS):
        put_scaled(k, (blocks[k].astype(F32) * natural[k]).astype(BF16))

    def rows(r, carry):
        at = pl.ds(pl.multiple_of(r * 8, 8), 8)
        put_errors(r, lattice([ybuf[at, s * LANES:(s + 1) * LANES] * permuted[s] for s in range(8)]))
        return carry

    lax.fori_loop(0, HB // 8, rows, 0, unroll=4)


def rotate_kernel(
    w_ref, lb_ref, rb_ref, g_ref, cos_ref,
    scaled_ref, err_ref, small_ref, last_ref, perm, cs_nat, cs_perm,
    wv, lb, rb, gv, cosv, had, mix, right, left, signed, inner, sb1, rb1, mid, rot, rb2, ybuf,
    gperm, pk_s, pk_r, e_s, e_r, t_s, t_r,
    w_sem, in_sem, s1_send, s1_recv, s2_send, s2_recv, pk_send, pk_recv, e_send, e_recv, t_send, t_recv,
):
    me = lax.axis_index("row")
    ex = lax.axis_index("expert")
    row_peer = [lax.rem(me + k, ROWS) for k in range(1, ROWS)]
    ex_peer = [
        {"expert": jnp.bitwise_xor(ex, ex_bit), "row": jnp.bitwise_xor(me, row_bit)} for ex_bit, row_bit in TOTAL_ORDER
    ]

    small_loads = [
        pltpu.make_async_copy(src, dst, in_sem.at[n])
        for n, (src, dst) in enumerate(((lb_ref, lb), (rb_ref, rb), (g_ref, gv), (cos_ref, cosv)))
    ]
    loads = [
        pltpu.make_async_copy(w_ref.at[0, pl.ds(i * HB, HB)], wv.at[pl.ds(i * HB, HB)], w_sem.at[i])
        for i in range(MINE)
    ]
    for load in small_loads[:2] + loads[:1]:
        load.start()
    barrier = pltpu.get_barrier_semaphore()
    for p in row_peer:
        pl.semaphore_signal(barrier, inc=1, device_id={"row": p}, device_id_type=MESH)
    for p in ex_peer:
        pl.semaphore_signal(barrier, inc=1, device_id=p, device_id_type=MESH)
    for load in loads[1:] + small_loads[2:]:
        load.start()

    had[...] = sign_of(jnp.bitwise_and(iota((256, 256), 0), iota((256, 256), 1)), 8).astype(BF16)
    small_loads[0].wait()
    small_loads[1].wait()
    right[...] = jnp.broadcast_to((2 * rb[...] - 1).astype(F32), (16, FF)).astype(BF16)

    def left_signs(i, carry):
        signs = (2 * lb[:, pl.ds(pl.multiple_of(i * HB, HB), HB)] - 1).astype(F32)
        left[i] = jnp.broadcast_to(signs, (HB, LANES)).T.astype(BF16)
        return carry

    left_signs(0, 0)

    def column_block(i):
        first = pl.multiple_of(i * HB, HB)
        lefts = jnp.concatenate([left[i], left[i]], axis=1)
        for p in range(8):
            x = wv[pl.ds(first, HB), p * 256:(p + 1) * 256]
            signed[p * HB:(p + 1) * HB, :] = x * lefts * right[0:1, p * 256:(p + 1) * 256]
        inner[...] = jnp.dot(signed[...], had[...], preferred_element_type=F32)
        for u in range(2):
            for r in range(HB // 16):
                parts = [inner[p * HB + r * 16:p * HB + (r + 1) * 16, u * LANES:(u + 1) * LANES] for p in range(8)]
                for t, part in enumerate(butterfly(parts)):
                    sb1[t // 4, (t % 4) * 2 + u, i, r * 16:(r + 1) * 16, :] = (part * (1.0 / math.sqrt(FF))).astype(BF16)

    def send_columns(i):
        for p in row_peer:
            push(sb1.at[0, p, i], rb1.at[0, me, i], s1_send.at[0], s1_recv.at[0], {"row": p})

    loads[0].wait()
    column_block(0)
    pl.semaphore_wait(barrier, ROWS - 1 + len(TOTAL_ORDER))
    send_columns(0)
    lax.fori_loop(1, MINE, left_signs, 0)

    def column_step(i, carry):
        pltpu.make_async_copy(w_ref.at[0, pl.ds(0, HB)], wv.at[pl.ds(0, HB)], w_sem.at[i]).wait()
        column_block(i)
        send_columns(i)
        return carry

    lax.fori_loop(1, MINE, column_step, 0)
    for p in row_peer:
        push(sb1.at[1, p], rb1.at[1, me], s1_send.at[1], s1_recv.at[1], {"row": p})
    for h in range(2):
        rb1[h, me] = sb1[h, me]

    small_loads[2].wait()
    small_loads[3].wait()
    pick_a = (jnp.right_shift(iota((896, 64), 0), 4) == iota((896, 64), 1)).astype(F32).astype(BF16)
    spread = jnp.dot(pick_a, cosv[...], preferred_element_type=F32).astype(BF16)
    pick_j = (jnp.right_shift(iota((LANES, 896), 1), 4) == iota((LANES, 896), 0)).astype(F32).astype(BF16)
    mix[...] = jnp.dot(spread, pick_j, preferred_element_type=F32).astype(BF16)
    small = sign_of(
        jnp.bitwise_and(jnp.bitwise_and(iota((16, 896), 0), iota((16, 896), 1)), 15), 4
    ).astype(BF16)

    def sign_mix(a, carry):
        at = pl.ds(pl.multiple_of(a * 16, 16), 16)
        mix[at, :] = mix[at, :] * small
        return carry

    lax.fori_loop(0, BLOCKS, sign_mix, 0)
    for s in range(8):
        perm[:, s * LANES:(s + 1) * LANES] = (
            iota((1024, LANES), 0) == 8 * iota((1024, LANES), 1) + s
        ).astype(F32).astype(BF16)
    which = iota((16, 1024), 0)
    ids = jnp.zeros((16, 1024), F32)
    for h in range(2):
        ids = jnp.where(which == h, gv[:, h * 1024:(h + 1) * 1024].astype(F32), ids)
        own = gv[:, pl.ds(pl.multiple_of(h * 1024 + me * LANES, LANES), LANES)].astype(F32)
        ids = jnp.where(which == 2 + h, jnp.concatenate([own] * 8, axis=1), ids)
    gperm[...] = jnp.dot(ids.astype(BF16), perm[...], preferred_element_type=F32)

    def rotate_rows(h):
        arrived(rb1.at[h, pl.ds(0, ROWS - 1)], s1_recv.at[h])

        def mix_blocks(q, carry):
            parts = []
            for half in range(2):
                at = pl.ds(pl.multiple_of(q * 32 + half * 16, 16), 16)
                parts.append(rb1[h, :, :, at, :].reshape(896, LANES))
            out = jnp.dot(mix[...], jnp.concatenate(parts, axis=1), preferred_element_type=F32)
            mid[2 * q] = out[:, :LANES]
            mid[2 * q + 1] = out[:, LANES:]
            return carry

        lax.fori_loop(0, 4, mix_blocks, 0)

        def turn(a, peak):
            at = pl.ds(pl.multiple_of(a * 16, 16), 16)
            parts = butterfly([mid[q, at, :] for q in range(8)])
            for q, part in enumerate(parts):
                part = part * (1.0 / math.sqrt(HB))
                peak = jnp.maximum(peak, jnp.abs(part))
                rot[h, a // MINE, lax.rem(a, MINE), q * 16:(q + 1) * 16, :] = part.astype(BF16)
            return peak

        peak = lax.fori_loop(0, BLOCKS, turn, jnp.zeros((16, LANES), F32))
        rb2[h, me] = rot[h, me]
        return jnp.max(peak, axis=0, keepdims=True)

    def send_rows(h, blocks):
        for i in blocks:
            for p in row_peer:
                push(rot.at[h, p, i], rb2.at[h, me, i], s2_send.at[h], s2_recv.at[h, i], {"row": p})

    def to_row(slots, own, source, send, recv):
        slots[me] = own
        source[...] = own
        for p in row_peer:
            push(source, slots.at[me], send, recv, {"row": p})

    col_peak = [rotate_rows(0)]
    send_rows(0, range(0, FIRST))
    col_peak.append(rotate_rows(1))

    group_id = iota((GROUPS, LANES), 0)
    most = jnp.zeros((GROUPS, LANES), F32)
    for h in range(2):
        own = gv[:, pl.ds(pl.multiple_of(h * 1024 + me * LANES, LANES), LANES)]
        most = jnp.maximum(most, jnp.where(group_id == own, col_peak[h], 0.0))
    most = jnp.broadcast_to(jnp.max(most, axis=1, keepdims=True), (GROUPS, LANES))
    to_row(pk_r, most, pk_s, pk_send, pk_recv)
    send_rows(0, range(FIRST, MINE))

    arrived(pk_r.at[pl.ds(0, ROWS - 1)], pk_recv)
    group_peak = jnp.ones((GROUPS, LANES), F32)
    for k in range(ROWS):
        group_peak = jnp.maximum(group_peak, pk_r[k])
    small_ref[0:1, :] = jnp.sum(
        jnp.where(group_id == iota((GROUPS, LANES), 1), group_peak * 0.5, 0.0), axis=0, keepdims=True
    )
    inverse = 2.0 / group_peak
    for m in range(16):
        ids = gv[:, m * LANES:(m + 1) * LANES]
        cs_nat[m:m + 1, :] = jnp.sum(jnp.where(group_id == ids, inverse, 0.0), axis=0, keepdims=True)
    for k in range(4):
        for s in range(8):
            ids = gperm[k:k + 1, s * LANES:(s + 1) * LANES]
            cs_perm[k, s:s + 1, :] = jnp.sum(
                jnp.where(group_id.astype(F32) == ids, inverse, 0.0), axis=0, keepdims=True
            )

    def own_errors(n, total):
        parts = []
        for h in range(2):
            blocks = []
            for k in range(8):
                a = n * 8 + k
                blocks.append(rot[h, a // MINE, lax.rem(a, MINE)])
            parts.append(jnp.concatenate(blocks, axis=1))
        ybuf[...] = jnp.dot(jnp.concatenate(parts, axis=0), perm[...], preferred_element_type=F32)
        block = n * 8 + jnp.right_shift(iota((8, LANES), 1), 4)
        for h in range(2):
            scales = [cs_perm[2 + h, s:s + 1, :] for s in range(8)]

            def rows(r, total):
                at = pl.ds(pl.multiple_of(h * HB + r * 8, 8), 8)
                errors = lattice([ybuf[at, s * LANES:(s + 1) * LANES] * scales[s] for s in range(8)])
                row = (block * HB + r * 8 + iota((8, LANES), 0)).astype(F32)
                return total + errors * ((1.0 + 4.0 * (row + 0.5) / D) / 3.0)

            total = lax.fori_loop(0, HB // 8, rows, total, unroll=4)
        return total

    error = lax.fori_loop(0, MIDDLE, own_errors, jnp.zeros((8, LANES), F32))
    error = lax.fori_loop(MIDDLE, MINE, own_errors, error)
    to_row(e_r, error, e_s, e_send, e_recv)
    send_rows(1, range(0, MINE))

    def finish(h, start, stop):
        def step(i, carry):
            arrived(rb2.at[h, pl.ds(0, ROWS - 1), i], s2_recv.at[h, i])
            first = pl.multiple_of(i * HB, HB)

            def put_scaled(k, value):
                scaled_ref[0, pl.ds(first, HB), (h * 8 + k) * LANES:(h * 8 + k + 1) * LANES] = value

            def put_errors(r, value):
                err_ref[0, pl.ds(pl.multiple_of(first + r * 8, 8), 8), h * LANES:(h + 1) * LANES] = value

            finish_block(
                [rb2[h, k, i] for k in range(ROWS)], perm, ybuf,
                [cs_nat[h * 8 + k:h * 8 + k + 1, :] for k in range(ROWS)],
                [cs_perm[h, s:s + 1, :] for s in range(8)], put_scaled, put_errors,
            )
            return carry

        lax.fori_loop(start, stop, step, 0)

    finish(0, 0, 2)
    arrived(e_r.at[pl.ds(0, ROWS - 1)], e_recv)
    error = e_r[0]
    for k in range(1, ROWS):
        error = error + e_r[k]
    error = jnp.sum(jnp.sum(error, axis=1, keepdims=True), axis=0, keepdims=True) * (1.0 / (D * FF // 8))
    total = jnp.broadcast_to(error, (8, LANES))
    small_ref[1:2, :] = total[:1]
    done = 2
    for n, p in enumerate(ex_peer):
        t_s[n] = total
        push(t_s.at[n], t_r.at[n], t_send.at[n], t_recv.at[n], p)
        more = 2 if n == 0 else 1
        finish(0, done, done + more)
        done += more
        arrived(t_r.at[n], t_recv.at[n])
        total = total + t_r[n]
    small_ref[2:3, :] = total[:1] * (1.0 / PEERS)
    finish(1, 0, MINE - 1)
    arrived(rb2.at[1, pl.ds(0, ROWS - 1), MINE - 1], s2_recv.at[1, MINE - 1])
    for k in range(ROWS):
        last_ref[k] = rb2[1, k, MINE - 1]

    for h in range(2):
        arrived(sb1.at[h, pl.ds(0, ROWS - 1)], s1_send.at[h])
        arrived(rot.at[h, pl.ds(0, ROWS - 1)], s2_send.at[h])
    arrived(pk_r.at[pl.ds(0, ROWS - 1)], pk_send)
    arrived(e_r.at[pl.ds(0, ROWS - 1)], e_send)
    for n in range(len(TOTAL_ORDER)):
        arrived(t_s.at[n], t_send.at[n])


def finish_kernel(
    scaled, errors, small, last, perm, cs_nat, cs_perm,
    scaled_ref, err_ref, scale_ref, expert_ref, total_ref,
    ybuf, scaled_last, err_last, sems,
):
    edge = (MINE - 1) * HB
    half = FF // 2
    copies = [
        pltpu.make_async_copy(scaled.at[:, pl.ds(0, edge)], scaled_ref.at[:, pl.ds(0, edge)], sems.at[0]),
        pltpu.make_async_copy(
            scaled.at[:, pl.ds(edge, HB), pl.ds(0, half)], scaled_ref.at[:, pl.ds(edge, HB), pl.ds(0, half)], sems.at[1]
        ),
        pltpu.make_async_copy(errors.at[:, pl.ds(0, edge)], err_ref.at[:, pl.ds(0, edge)], sems.at[2]),
        pltpu.make_async_copy(
            errors.at[:, pl.ds(edge, HB), pl.ds(0, LANES)], err_ref.at[:, pl.ds(edge, HB), pl.ds(0, LANES)], sems.at[3]
        ),
    ]
    for copy in copies:
        copy.start()
    scale_ref[...] = small[0:1, :GROUPS]
    expert_ref[...] = small[1:2, :1]
    total_ref[...] = small[2:3, :1]

    def put_scaled(k, value):
        scaled_last[0, :, k * LANES:(k + 1) * LANES] = value

    def put_errors(r, value):
        err_last[0, pl.ds(pl.multiple_of(r * 8, 8), 8), :] = value

    finish_block(
        [last[k] for k in range(ROWS)], perm, ybuf,
        [cs_nat[8 + k:9 + k, :] for k in range(ROWS)],
        [cs_perm[1, s:s + 1, :] for s in range(8)], put_scaled, put_errors,
    )
    rest = [
        pltpu.make_async_copy(scaled_last, scaled_ref.at[:, pl.ds(edge, HB), pl.ds(half, half)], sems.at[4]),
        pltpu.make_async_copy(err_last, err_ref.at[:, pl.ds(edge, HB), pl.ds(LANES, LANES)], sems.at[5]),
    ]
    for copy in rest:
        copy.start()
    for copy in copies + rest:
        copy.wait()


def body(weights, left_bits, right_bits, groups):
    vmem = pl.BlockSpec(memory_space=pltpu.VMEM)
    hbm = pl.BlockSpec(memory_space=pltpu.HBM)
    rows = MINE * HB
    dma = pltpu.SemaphoreType.DMA
    arguments = [
        pltpu.with_memory_space_constraint(x, pltpu.HBM)
        for x in (weights, left_bits, right_bits, groups, jnp.asarray(cosine_table()))
    ]
    parts = pl.pallas_call(
        rotate_kernel,
        out_shape=(
            pltpu.VMEM((1, rows, FF), BF16),
            pltpu.VMEM((1, rows, FF // 8), F32),
            pltpu.VMEM((8, LANES), F32),
            pltpu.VMEM((ROWS, HB, LANES), BF16),
            pltpu.VMEM((1024, 1024), BF16),
            pltpu.VMEM((16, LANES), F32),
            pltpu.VMEM((4, 8, LANES), F32),
        ),
        in_specs=[hbm] * 5,
        out_specs=(vmem,) * 7,
        scratch_shapes=[
            pltpu.VMEM((rows, FF), BF16),
            pltpu.VMEM((1, rows), jnp.int32),
            pltpu.VMEM((1, FF), jnp.int32),
            pltpu.VMEM((1, FF), jnp.int32),
            pltpu.VMEM((64, LANES), BF16),
            pltpu.VMEM((256, 256), BF16),
            pltpu.VMEM((896, 896), BF16),
            pltpu.VMEM((16, FF), BF16),
            pltpu.VMEM((MINE, HB, LANES), BF16),
            pltpu.VMEM((8 * HB, 256), BF16),
            pltpu.VMEM((8 * HB, 256), F32),
            pltpu.VMEM((2, ROWS, MINE, HB, LANES), BF16),
            pltpu.VMEM((2, ROWS, MINE, HB, LANES), BF16),
            pltpu.VMEM((8, 896, LANES), F32),
            pltpu.VMEM((2, ROWS, MINE, HB, LANES), BF16),
            pltpu.VMEM((2, ROWS, MINE, HB, LANES), BF16),
            pltpu.VMEM((2 * HB, 1024), F32),
            pltpu.VMEM((16, 1024), F32),
            pltpu.VMEM((GROUPS, LANES), F32),
            pltpu.VMEM((ROWS, GROUPS, LANES), F32),
            pltpu.VMEM((8, LANES), F32),
            pltpu.VMEM((ROWS, 8, LANES), F32),
            pltpu.VMEM((len(TOTAL_ORDER), 8, LANES), F32),
            pltpu.VMEM((len(TOTAL_ORDER), 8, LANES), F32),
            dma((MINE,)),
            dma((4,)),
            dma((2,)),
            dma((2,)),
            dma((2,)),
            dma((2, MINE)),
            dma,
            dma,
            dma,
            dma,
            dma((len(TOTAL_ORDER),)),
            dma((len(TOTAL_ORDER),)),
        ],
        compiler_params=pltpu.CompilerParams(
            collective_id=0, has_side_effects=True, vmem_limit_bytes=VMEM_LIMIT
        ),
        name="rotate",
    )(*arguments)
    scaled, errors, scales, expert_error, total_error = pl.pallas_call(
        finish_kernel,
        out_shape=(
            jax.ShapeDtypeStruct((1, rows, FF), BF16),
            jax.ShapeDtypeStruct((1, rows, FF // 8), F32),
            jax.ShapeDtypeStruct((1, GROUPS), F32),
            jax.ShapeDtypeStruct((1, 1), F32),
            jax.ShapeDtypeStruct((1, 1), F32),
        ),
        in_specs=[vmem] * 7,
        out_specs=(hbm, hbm, vmem, vmem, vmem),
        scratch_shapes=[
            pltpu.VMEM((HB, 1024), F32),
            pltpu.VMEM((1, HB, FF // 2), BF16),
            pltpu.VMEM((1, HB, LANES), F32),
            dma((6,)),
        ],
        compiler_params=pltpu.CompilerParams(vmem_limit_bytes=8 * 2**20),
        name="finish",
    )(*parts)
    return scaled, errors, scales, expert_error.reshape(1), total_error.reshape(())


def solution(mesh):
    placed = (P("expert", "row", None), P("expert", "row"), P("expert", None), P("expert", None))
    return jax.shard_map(
        body,
        mesh=mesh,
        in_specs=placed,
        out_specs=(
            P("expert", "row", None),
            P("expert", "row", None),
            P("expert", None),
            P("expert"),
            P(),
        ),
        check_vma=False,
    )
```

```python
import math

import jax
import jax.numpy as jnp
import ml_dtypes
import numpy as np
from jax import lax
from jax.experimental import pallas as pl
from jax.experimental.pallas import tpu as pltpu
from jax.sharding import PartitionSpec as P

D = 7168
FF = 2048
HB = 128
GROUPS = 16
BLOCKS = 56
ROWS = 8
PEERS = 16
MINE = BLOCKS // ROWS
LANES = 128
MESH = pl.DeviceIdType.MESH
TOTAL_ORDER = ((8, 1), (1, 0), (2, 0), (4, 0))
FIRST = 3
MIDDLE = 4
VMEM_LIMIT = 56 * 2**20
F32 = jnp.float32
BF16 = jnp.bfloat16


def cosine_table():
    first = np.arange(BLOCKS, dtype=np.float64)[:, None]
    second = np.arange(BLOCKS, dtype=np.float64)[None, :]
    table = math.sqrt(2.0 / BLOCKS) * np.cos(math.pi * (2.0 * second + 1.0) * first / (2.0 * BLOCKS))
    table[0] *= math.sqrt(0.5)
    padded = np.zeros((64, LANES), np.float32)
    padded[:BLOCKS, :BLOCKS] = table
    return padded.astype(ml_dtypes.bfloat16)


def iota(shape, dim):
    return lax.broadcasted_iota(jnp.int32, shape, dim)


def sign_of(common, bits):
    parity = common
    shift = bits // 2
    while shift:
        parity = jnp.bitwise_xor(parity, jnp.right_shift(parity, shift))
        shift //= 2
    return (1 - 2 * jnp.bitwise_and(parity, 1)).astype(F32)


def butterfly(parts):
    parts = list(parts)
    step = 1
    while step < len(parts):
        for low in range(len(parts)):
            if not low & step:
                a, b = parts[low], parts[low + step]
                parts[low], parts[low + step] = a + b, a - b
        step *= 2
    return parts


def odd(count):
    return count - 2.0 * jnp.floor(count * 0.5) > 0.5


def lattice(values):
    first = None
    for value in values:
        whole = jnp.floor(value)
        g = jnp.abs((value - whole) - 0.5)
        near = jnp.floor(value + 0.5)
        now = (g, g * g, g, g, whole, near)
        if first is None:
            first = now
        else:
            first = (
                first[0] + now[0],
                first[1] + now[1],
                jnp.maximum(first[2], g),
                jnp.minimum(first[3], g),
                first[4] + whole,
                first[5] + near,
            )
    total, squares, most, least, halves, wholes = first
    shifted = jnp.where(odd(halves), squares + 1.0 - 2.0 * most, squares)
    plain = 2.0 - total + squares
    plain = jnp.where(odd(wholes), plain + 2.0 * least, plain)
    return jnp.minimum(plain, shifted)


def push(src, dst, send, recv, device):
    pltpu.make_async_remote_copy(src, dst, send, recv, device_id=device, device_id_type=MESH).start()


def arrived(ref, sem):
    pltpu.make_async_copy(ref, ref, sem).wait()


def finish_block(blocks, perm, ybuf, natural, permuted, put_scaled, put_errors):
    ybuf[:HB, :] = jnp.dot(jnp.concatenate(blocks, axis=1), perm[...], preferred_element_type=F32)
    for k in range(ROWS):
        put_scaled(k, (blocks[k].astype(F32) * natural[k]).astype(BF16))

    def rows(r, carry):
        at = pl.ds(pl.multiple_of(r * 8, 8), 8)
        put_errors(r, lattice([ybuf[at, s * LANES:(s + 1) * LANES] * permuted[s] for s in range(8)]))
        return carry

    lax.fori_loop(0, HB // 8, rows, 0, unroll=8)


def rotate_kernel(
    w_ref, lb_ref, rb_ref, g_ref, cos_ref,
    scaled_ref, err_ref, small_ref, last_ref, perm, cs_nat, cs_perm,
    wv, lb, rb, gv, cosv, had, mix, right, left, signed, inner, sb1, rb1, mid, rot, rb2, ybuf,
    gperm, pk_s, pk_r, e_s, e_r, t_s, t_r,
    here, w_sem, in_sem, s1_send, s1_recv, s2_send, s2_recv, pk_send, pk_recv, e_send, e_recv, t_send, t_recv,
):
    me = lax.axis_index("row")
    ex = lax.axis_index("expert")
    row_peer = [
        lax.rem(jnp.right_shift(me, 1) + dz, 4) * 2 + jnp.bitwise_xor(jnp.bitwise_and(me, 1), dx)
        for dz, dx in ((2, 1), (2, 0), (1, 1), (3, 1), (1, 0), (3, 0), (0, 1))
    ]
    ex_peer = [
        {"expert": jnp.bitwise_xor(ex, ex_bit), "row": jnp.bitwise_xor(me, row_bit)} for ex_bit, row_bit in TOTAL_ORDER
    ]

    small_loads = [
        pltpu.make_async_copy(src, dst, in_sem.at[n])
        for n, (src, dst) in enumerate(((lb_ref, lb), (rb_ref, rb), (g_ref, gv), (cos_ref, cosv)))
    ]
    loads = [
        pltpu.make_async_copy(w_ref.at[0, pl.ds(i * HB, HB)], wv.at[pl.ds(i * HB, HB)], w_sem.at[i])
        for i in range(MINE)
    ]
    for load in small_loads[:2] + loads[:1]:
        load.start()
    barrier = pltpu.get_barrier_semaphore()
    for p in row_peer:
        pl.semaphore_signal(barrier, inc=1, device_id={"row": p}, device_id_type=MESH)
    higher = [jnp.bitwise_and(ex, ex_bit) != 0 for ex_bit, _ in TOTAL_ORDER]
    for p, high in zip(ex_peer, higher):

        @pl.when(jnp.logical_not(high))
        def _():
            pl.semaphore_signal(barrier, inc=1, device_id=p, device_id_type=MESH)

    for load in loads[1:] + small_loads[2:]:
        load.start()

    had[...] = sign_of(jnp.bitwise_and(iota((256, 256), 0), iota((256, 256), 1)), 8).astype(BF16)
    small_loads[0].wait()
    small_loads[1].wait()
    right[...] = jnp.broadcast_to((2 * rb[...] - 1).astype(F32), (16, FF)).astype(BF16)

    def left_signs(i, carry):
        signs = (2 * lb[:, pl.ds(pl.multiple_of(i * HB, HB), HB)] - 1).astype(F32)
        left[i] = jnp.broadcast_to(signs, (HB, LANES)).T.astype(BF16)
        return carry

    left_signs(0, 0)

    def column_block(i):
        first = pl.multiple_of(i * HB, HB)
        lefts = jnp.concatenate([left[i], left[i]], axis=1)
        for p in range(8):
            x = wv[pl.ds(first, HB), p * 256:(p + 1) * 256]
            signed[p * HB:(p + 1) * HB, :] = x * lefts * right[0:1, p * 256:(p + 1) * 256]
        inner[...] = jnp.dot(signed[...], had[...], preferred_element_type=F32)
        for u in range(2):
            for r in range(HB // 16):
                parts = [inner[p * HB + r * 16:p * HB + (r + 1) * 16, u * LANES:(u + 1) * LANES] for p in range(8)]
                for t, part in enumerate(butterfly(parts)):
                    sb1[t // 4, (t % 4) * 2 + u, i, r * 16:(r + 1) * 16, :] = (part * (1.0 / math.sqrt(FF))).astype(BF16)

    def send_columns(i):
        for p in row_peer:
            push(sb1.at[0, p, i], rb1.at[0, me, i], s1_send.at[0], s1_recv.at[0], {"row": p})

    loads[0].wait()
    column_block(0)
    pl.semaphore_wait(barrier, ROWS - 1 + sum(high.astype(jnp.int32) for high in higher))
    send_columns(0)
    lax.fori_loop(1, MINE, left_signs, 0)

    def column_step(i, carry):
        pltpu.make_async_copy(w_ref.at[0, pl.ds(0, HB)], wv.at[pl.ds(0, HB)], w_sem.at[i]).wait()
        column_block(i)
        send_columns(i)
        return carry

    lax.fori_loop(1, MINE, column_step, 0)
    for p in row_peer:
        push(sb1.at[1, p], rb1.at[1, me], s1_send.at[1], s1_recv.at[1], {"row": p})
    for n, (p, high) in enumerate(zip(ex_peer, higher)):

        @pl.when(high)
        def _():
            pl.semaphore_signal(here.at[n], inc=1, device_id=p, device_id_type=MESH)

    for h in range(2):
        rb1[h, me] = sb1[h, me]

    small_loads[2].wait()
    small_loads[3].wait()
    pick_a = (jnp.right_shift(iota((896, 64), 0), 4) == iota((896, 64), 1)).astype(F32).astype(BF16)
    spread = jnp.dot(pick_a, cosv[...], preferred_element_type=F32).astype(BF16)
    pick_j = (jnp.right_shift(iota((LANES, 896), 1), 4) == iota((LANES, 896), 0)).astype(F32).astype(BF16)
    mix[...] = jnp.dot(spread, pick_j, preferred_element_type=F32).astype(BF16)
    small = sign_of(
        jnp.bitwise_and(jnp.bitwise_and(iota((16, 896), 0), iota((16, 896), 1)), 15), 4
    ).astype(BF16)

    def sign_mix(a, carry):
        at = pl.ds(pl.multiple_of(a * 16, 16), 16)
        mix[at, :] = mix[at, :] * small
        return carry

    lax.fori_loop(0, BLOCKS, sign_mix, 0)
    for s in range(8):
        perm[:, s * LANES:(s + 1) * LANES] = (
            iota((1024, LANES), 0) == 8 * iota((1024, LANES), 1) + s
        ).astype(F32).astype(BF16)
    which = iota((16, 1024), 0)
    ids = jnp.zeros((16, 1024), F32)
    for h in range(2):
        ids = jnp.where(which == h, gv[:, h * 1024:(h + 1) * 1024].astype(F32), ids)
        own = gv[:, pl.ds(pl.multiple_of(h * 1024 + me * LANES, LANES), LANES)].astype(F32)
        ids = jnp.where(which == 2 + h, jnp.concatenate([own] * 8, axis=1), ids)
    gperm[...] = jnp.dot(ids.astype(BF16), perm[...], preferred_element_type=F32)

    def rotate_rows(h):
        arrived(rb1.at[h, pl.ds(0, ROWS - 1)], s1_recv.at[h])

        def mix_blocks(q, carry):
            parts = []
            for half in range(2):
                at = pl.ds(pl.multiple_of(q * 32 + half * 16, 16), 16)
                parts.append(rb1[h, :, :, at, :].reshape(896, LANES))
            out = jnp.dot(mix[...], jnp.concatenate(parts, axis=1), preferred_element_type=F32)
            mid[2 * q] = out[:, :LANES]
            mid[2 * q + 1] = out[:, LANES:]
            return carry

        lax.fori_loop(0, 4, mix_blocks, 0)

        def turn(a, peak):
            at = pl.ds(pl.multiple_of(a * 16, 16), 16)
            parts = butterfly([mid[q, at, :] for q in range(8)])
            for q, part in enumerate(parts):
                part = part * (1.0 / math.sqrt(HB))
                peak = jnp.maximum(peak, jnp.abs(part))
                rot[h, a // MINE, lax.rem(a, MINE), q * 16:(q + 1) * 16, :] = part.astype(BF16)
            return peak

        peak = lax.fori_loop(0, BLOCKS, turn, jnp.zeros((16, LANES), F32), unroll=4)
        rb2[h, me] = rot[h, me]
        return jnp.max(peak, axis=0, keepdims=True)

    def send_rows(h, blocks):
        for i in blocks:
            for p in row_peer:
                push(rot.at[h, p, i], rb2.at[h, me, i], s2_send.at[h], s2_recv.at[h, i], {"row": p})

    def to_row(slots, own, source, send, recv):
        slots[me] = own
        source[...] = own
        for p in row_peer:
            push(source, slots.at[me], send, recv, {"row": p})

    col_peak = [rotate_rows(0)]
    send_rows(0, range(0, FIRST))
    col_peak.append(rotate_rows(1))

    group_id = iota((GROUPS, LANES), 0)
    most = jnp.zeros((GROUPS, LANES), F32)
    for h in range(2):
        own = gv[:, pl.ds(pl.multiple_of(h * 1024 + me * LANES, LANES), LANES)]
        most = jnp.maximum(most, jnp.where(group_id == own, col_peak[h], 0.0))
    most = jnp.broadcast_to(jnp.max(most, axis=1, keepdims=True), (GROUPS, LANES))
    to_row(pk_r, most, pk_s, pk_send, pk_recv)
    send_rows(0, range(FIRST, MINE))

    arrived(pk_r.at[pl.ds(0, ROWS - 1)], pk_recv)
    group_peak = jnp.ones((GROUPS, LANES), F32)
    for k in range(ROWS):
        group_peak = jnp.maximum(group_peak, pk_r[k])
    small_ref[0:1, :] = jnp.sum(
        jnp.where(group_id == iota((GROUPS, LANES), 1), group_peak * 0.5, 0.0), axis=0, keepdims=True
    )
    inverse = 2.0 / group_peak
    for m in range(16):
        ids = gv[:, m * LANES:(m + 1) * LANES]
        cs_nat[m:m + 1, :] = jnp.sum(jnp.where(group_id == ids, inverse, 0.0), axis=0, keepdims=True)
    for k in range(4):
        for s in range(8):
            ids = gperm[k:k + 1, s * LANES:(s + 1) * LANES]
            cs_perm[k, s:s + 1, :] = jnp.sum(
                jnp.where(group_id.astype(F32) == ids, inverse, 0.0), axis=0, keepdims=True
            )

    def reorder(n):
        parts = []
        for h in range(2):
            blocks = [rot[h, (n * 8 + k) // MINE, (n * 8 + k) % MINE] for k in range(8)]
            parts.append(jnp.concatenate(blocks, axis=1))
        return jnp.dot(jnp.concatenate(parts, axis=0), perm[...], preferred_element_type=F32)

    def own_errors(n, total):
        block = n * 8 + jnp.right_shift(iota((8, LANES), 1), 4)
        for h in range(2):
            scales = [cs_perm[2 + h, s:s + 1, :] for s in range(8)]
            for r in range(HB // 8):
                at = slice(h * HB + r * 8, h * HB + r * 8 + 8)
                errors = lattice([ybuf[n % 2, at, s * LANES:(s + 1) * LANES] * scales[s] for s in range(8)])
                row = (block * HB + r * 8 + iota((8, LANES), 0)).astype(F32)
                total = total + errors * ((1.0 + 4.0 * (row + 0.5) / D) / 3.0)
        return total

    error = jnp.zeros((8, LANES), F32)
    ybuf[0] = reorder(0)
    for n in range(MINE):
        if n + 1 < MINE:
            ybuf[(n + 1) % 2] = reorder(n + 1)
        error = own_errors(n, error)
    to_row(e_r, error, e_s, e_send, e_recv)
    send_rows(1, range(0, MINE))

    def finish(h, start, stop):
        def step(i, carry):
            arrived(rb2.at[h, pl.ds(0, ROWS - 1), i], s2_recv.at[h, i])
            first = pl.multiple_of(i * HB, HB)

            def put_scaled(k, value):
                scaled_ref[0, pl.ds(first, HB), (h * 8 + k) * LANES:(h * 8 + k + 1) * LANES] = value

            def put_errors(r, value):
                err_ref[0, pl.ds(pl.multiple_of(first + r * 8, 8), 8), h * LANES:(h + 1) * LANES] = value

            finish_block(
                [rb2[h, k, i] for k in range(ROWS)], perm, ybuf.at[0],
                [cs_nat[h * 8 + k:h * 8 + k + 1, :] for k in range(ROWS)],
                [cs_perm[h, s:s + 1, :] for s in range(8)], put_scaled, put_errors,
            )
            return carry

        lax.fori_loop(start, stop, step, 0)

    finish(0, 0, 4)
    arrived(e_r.at[pl.ds(0, ROWS - 1)], e_recv)
    error = e_r[0]
    for k in range(1, ROWS):
        error = error + e_r[k]
    error = jnp.sum(jnp.sum(error, axis=1, keepdims=True), axis=0, keepdims=True) * (1.0 / (D * FF // 8))
    total = jnp.broadcast_to(error, (8, LANES))
    small_ref[1:2, :] = total[:1]
    meanwhile = ((0, 4, MINE), (1, 0, 1), (1, 1, 2), (1, 2, MINE - 1))
    for n, p in enumerate(ex_peer):
        t_s[n] = total

        @pl.when(jnp.logical_not(higher[n]))
        def _():
            pl.semaphore_wait(here.at[n], 1)

        push(t_s.at[n], t_r.at[n], t_send.at[n], t_recv.at[n], p)
        finish(*meanwhile[n])
        arrived(t_r.at[n], t_recv.at[n])
        total = total + t_r[n]
    small_ref[2:3, :] = total[:1] * (1.0 / PEERS)
    arrived(rb2.at[1, pl.ds(0, ROWS - 1), MINE - 1], s2_recv.at[1, MINE - 1])
    for k in range(ROWS):
        last_ref[k] = rb2[1, k, MINE - 1]

    for h in range(2):
        arrived(sb1.at[h, pl.ds(0, ROWS - 1)], s1_send.at[h])
        arrived(rot.at[h, pl.ds(0, ROWS - 1)], s2_send.at[h])
    arrived(pk_r.at[pl.ds(0, ROWS - 1)], pk_send)
    arrived(e_r.at[pl.ds(0, ROWS - 1)], e_send)
    for n in range(len(TOTAL_ORDER)):
        arrived(t_s.at[n], t_send.at[n])


def finish_kernel(
    scaled, errors, small, last, perm, cs_nat, cs_perm,
    scaled_ref, err_ref, scale_ref, expert_ref, total_ref,
    ybuf, scaled_last, err_last, scale_v, expert_v, total_v, sems,
):
    edge = (MINE - 1) * HB
    half = FF // 2
    copies = [
        pltpu.make_async_copy(scaled.at[:, pl.ds(0, edge)], scaled_ref.at[:, pl.ds(0, edge)], sems.at[0]),
        pltpu.make_async_copy(
            scaled.at[:, pl.ds(edge, HB), pl.ds(0, half)], scaled_ref.at[:, pl.ds(edge, HB), pl.ds(0, half)], sems.at[1]
        ),
        pltpu.make_async_copy(errors.at[:, pl.ds(0, edge)], err_ref.at[:, pl.ds(0, edge)], sems.at[2]),
        pltpu.make_async_copy(
            errors.at[:, pl.ds(edge, HB), pl.ds(0, LANES)], err_ref.at[:, pl.ds(edge, HB), pl.ds(0, LANES)], sems.at[3]
        ),
    ]
    for copy in copies:
        copy.start()
    scale_v[...] = small[0:1, :GROUPS]
    expert_v[...] = small[1:2, :1]
    total_v[...] = small[2:3, :1]
    for n, (src, dst) in enumerate(((scale_v, scale_ref), (expert_v, expert_ref), (total_v, total_ref))):
        copies.append(pltpu.make_async_copy(src, dst, sems.at[6 + n]))
        copies[-1].start()

    def put_scaled(k, value):
        scaled_last[0, :, k * LANES:(k + 1) * LANES] = value

    def put_errors(r, value):
        err_last[0, pl.ds(pl.multiple_of(r * 8, 8), 8), :] = value

    finish_block(
        [last[k] for k in range(ROWS)], perm, ybuf,
        [cs_nat[8 + k:9 + k, :] for k in range(ROWS)],
        [cs_perm[1, s:s + 1, :] for s in range(8)], put_scaled, put_errors,
    )
    rest = [
        pltpu.make_async_copy(scaled_last, scaled_ref.at[:, pl.ds(edge, HB), pl.ds(half, half)], sems.at[4]),
        pltpu.make_async_copy(err_last, err_ref.at[:, pl.ds(edge, HB), pl.ds(LANES, LANES)], sems.at[5]),
    ]
    for copy in rest:
        copy.start()
    for copy in copies + rest:
        copy.wait()


def body(weights, left_bits, right_bits, groups):
    vmem = pl.BlockSpec(memory_space=pltpu.VMEM)
    hbm = pl.BlockSpec(memory_space=pltpu.HBM)
    rows = MINE * HB
    dma = pltpu.SemaphoreType.DMA
    arguments = [
        pltpu.with_memory_space_constraint(x, pltpu.HBM)
        for x in (weights, left_bits, right_bits, groups, jnp.asarray(cosine_table()))
    ]
    parts = pl.pallas_call(
        rotate_kernel,
        out_shape=(
            pltpu.VMEM((1, rows, FF), BF16),
            pltpu.VMEM((1, rows, FF // 8), F32),
            pltpu.VMEM((8, LANES), F32),
            pltpu.VMEM((ROWS, HB, LANES), BF16),
            pltpu.VMEM((1024, 1024), BF16),
            pltpu.VMEM((16, LANES), F32),
            pltpu.VMEM((4, 8, LANES), F32),
        ),
        in_specs=[hbm] * 5,
        out_specs=(vmem,) * 7,
        scratch_shapes=[
            pltpu.VMEM((rows, FF), BF16),
            pltpu.VMEM((1, rows), jnp.int32),
            pltpu.VMEM((1, FF), jnp.int32),
            pltpu.VMEM((1, FF), jnp.int32),
            pltpu.VMEM((64, LANES), BF16),
            pltpu.VMEM((256, 256), BF16),
            pltpu.VMEM((896, 896), BF16),
            pltpu.VMEM((16, FF), BF16),
            pltpu.VMEM((MINE, HB, LANES), BF16),
            pltpu.VMEM((8 * HB, 256), BF16),
            pltpu.VMEM((8 * HB, 256), F32),
            pltpu.VMEM((2, ROWS, MINE, HB, LANES), BF16),
            pltpu.VMEM((2, ROWS, MINE, HB, LANES), BF16),
            pltpu.VMEM((8, 896, LANES), F32),
            pltpu.VMEM((2, ROWS, MINE, HB, LANES), BF16),
            pltpu.VMEM((2, ROWS, MINE, HB, LANES), BF16),
            pltpu.VMEM((2, 2 * HB, 1024), F32),
            pltpu.VMEM((16, 1024), F32),
            pltpu.VMEM((GROUPS, LANES), F32),
            pltpu.VMEM((ROWS, GROUPS, LANES), F32),
            pltpu.VMEM((8, LANES), F32),
            pltpu.VMEM((ROWS, 8, LANES), F32),
            pltpu.VMEM((len(TOTAL_ORDER), 8, LANES), F32),
            pltpu.VMEM((len(TOTAL_ORDER), 8, LANES), F32),
            pltpu.SemaphoreType.REGULAR((len(TOTAL_ORDER),)),
            dma((MINE,)),
            dma((4,)),
            dma((2,)),
            dma((2,)),
            dma((2,)),
            dma((2, MINE)),
            dma,
            dma,
            dma,
            dma,
            dma((len(TOTAL_ORDER),)),
            dma((len(TOTAL_ORDER),)),
        ],
        compiler_params=pltpu.CompilerParams(
            collective_id=0, has_side_effects=True, vmem_limit_bytes=VMEM_LIMIT
        ),
        name="rotate",
    )(*arguments)
    scaled, errors, scales, expert_error, total_error = pl.pallas_call(
        finish_kernel,
        out_shape=(
            jax.ShapeDtypeStruct((1, rows, FF), BF16),
            jax.ShapeDtypeStruct((1, rows, FF // 8), F32),
            jax.ShapeDtypeStruct((1, GROUPS), F32),
            jax.ShapeDtypeStruct((1, 1), F32),
            jax.ShapeDtypeStruct((1, 1), F32),
        ),
        in_specs=[vmem] * 7,
        out_specs=(hbm,) * 5,
        scratch_shapes=[
            pltpu.VMEM((HB, 1024), F32),
            pltpu.VMEM((1, HB, FF // 2), BF16),
            pltpu.VMEM((1, HB, LANES), F32),
            pltpu.VMEM((1, GROUPS), F32),
            pltpu.VMEM((1, 1), F32),
            pltpu.VMEM((1, 1), F32),
            dma((9,)),
        ],
        compiler_params=pltpu.CompilerParams(vmem_limit_bytes=8 * 2**20),
        name="finish",
    )(*parts)
    return scaled, errors, scales, expert_error.reshape(1), total_error.reshape(())


def solution(mesh):
    placed = (P("expert", "row", None), P("expert", "row"), P("expert", None), P("expert", None))
    return jax.shard_map(
        body,
        mesh=mesh,
        in_specs=placed,
        out_specs=(
            P("expert", "row", None),
            P("expert", "row", None),
            P("expert", None),
            P("expert"),
            P(),
        ),
        check_vma=False,
    )
```

```python
import math

import jax
import jax.numpy as jnp
import ml_dtypes
import numpy as np
from jax import lax
from jax.experimental import pallas as pl
from jax.experimental.pallas import tpu as pltpu
from jax.sharding import PartitionSpec as P

D = 7168
FF = 2048
HB = 128
GROUPS = 16
BLOCKS = 56
ROWS = 8
PEERS = 16
MINE = BLOCKS // ROWS
LANES = 128
MESH = pl.DeviceIdType.MESH
TOTAL_ORDER = ((8, 1), (1, 0), (2, 0), (4, 0))
FIRST = 3
MIDDLE = 4
VMEM_LIMIT = 56 * 2**20
F32 = jnp.float32
BF16 = jnp.bfloat16


def cosine_table():
    first = np.arange(BLOCKS, dtype=np.float64)[:, None]
    second = np.arange(BLOCKS, dtype=np.float64)[None, :]
    table = math.sqrt(2.0 / BLOCKS) * np.cos(math.pi * (2.0 * second + 1.0) * first / (2.0 * BLOCKS))
    table[0] *= math.sqrt(0.5)
    padded = np.zeros((64, LANES), np.float32)
    padded[:BLOCKS, :BLOCKS] = table
    return padded.astype(ml_dtypes.bfloat16)


def iota(shape, dim):
    return lax.broadcasted_iota(jnp.int32, shape, dim)


def sign_of(common, bits):
    parity = common
    shift = bits // 2
    while shift:
        parity = jnp.bitwise_xor(parity, jnp.right_shift(parity, shift))
        shift //= 2
    return (1 - 2 * jnp.bitwise_and(parity, 1)).astype(F32)


def butterfly(parts):
    parts = list(parts)
    step = 1
    while step < len(parts):
        for low in range(len(parts)):
            if not low & step:
                a, b = parts[low], parts[low + step]
                parts[low], parts[low + step] = a + b, a - b
        step *= 2
    return parts


def odd(count):
    return count - 2.0 * jnp.floor(count * 0.5) > 0.5


def lattice(values):
    first = None
    for value in values:
        whole = jnp.floor(value)
        g = jnp.abs((value - whole) - 0.5)
        near = jnp.floor(value + 0.5)
        now = (g, g * g, g, g, whole, near)
        if first is None:
            first = now
        else:
            first = (
                first[0] + now[0],
                first[1] + now[1],
                jnp.maximum(first[2], g),
                jnp.minimum(first[3], g),
                first[4] + whole,
                first[5] + near,
            )
    total, squares, most, least, halves, wholes = first
    shifted = jnp.where(odd(halves), squares + 1.0 - 2.0 * most, squares)
    plain = 2.0 - total + squares
    plain = jnp.where(odd(wholes), plain + 2.0 * least, plain)
    return jnp.minimum(plain, shifted)


def push(src, dst, send, recv, device):
    pltpu.make_async_remote_copy(src, dst, send, recv, device_id=device, device_id_type=MESH).start()


def arrived(ref, sem):
    pltpu.make_async_copy(ref, ref, sem).wait()


def finish_block(blocks, perm, ybuf, natural, permuted, put_scaled, put_errors):
    ybuf[:HB, :] = jnp.dot(jnp.concatenate(blocks, axis=1), perm[...], preferred_element_type=F32)
    for k in range(ROWS):
        put_scaled(k, (blocks[k].astype(F32) * natural[k]).astype(BF16))

    def rows(r, carry):
        at = pl.ds(pl.multiple_of(r * 8, 8), 8)
        put_errors(r, lattice([ybuf[at, s * LANES:(s + 1) * LANES] * permuted[s] for s in range(8)]))
        return carry

    lax.fori_loop(0, HB // 8, rows, 0, unroll=8)


def rotate_kernel(
    w_ref, lb_ref, rb_ref, g_ref, cos_ref,
    scaled_ref, err_ref, small_ref, last_ref, perm, cs_nat, cs_perm,
    wv, lb, rb, gv, cosv, had, mix, right, left, signed, inner, sb1, rb1, mid, rot, rb2, ybuf,
    gperm, pk_s, pk_r, e_s, e_r, t_s, t_r,
    here, w_sem, in_sem, s1_send, s1_recv, s2_send, s2_recv, pk_send, pk_recv, e_send, e_recv, t_send, t_recv,
):
    me = lax.axis_index("row")
    ex = lax.axis_index("expert")
    row_peer = [
        lax.rem(jnp.right_shift(me, 1) + dz, 4) * 2 + jnp.bitwise_xor(jnp.bitwise_and(me, 1), dx)
        for dz, dx in ((2, 1), (2, 0), (1, 1), (3, 1), (1, 0), (3, 0), (0, 1))
    ]
    ex_peer = [
        {"expert": jnp.bitwise_xor(ex, ex_bit), "row": jnp.bitwise_xor(me, row_bit)} for ex_bit, row_bit in TOTAL_ORDER
    ]

    small_loads = [
        pltpu.make_async_copy(src, dst, in_sem.at[n])
        for n, (src, dst) in enumerate(((lb_ref, lb), (rb_ref, rb), (g_ref, gv), (cos_ref, cosv)))
    ]
    loads = [
        pltpu.make_async_copy(w_ref.at[0, pl.ds(i * HB, HB)], wv.at[pl.ds(i * HB, HB)], w_sem.at[i])
        for i in range(MINE)
    ]
    for load in small_loads[:2] + loads[:1]:
        load.start()
    barrier = pltpu.get_barrier_semaphore()
    for p in row_peer:
        pl.semaphore_signal(barrier, inc=1, device_id={"row": p}, device_id_type=MESH)
    higher = [jnp.bitwise_and(ex, ex_bit) != 0 for ex_bit, _ in TOTAL_ORDER]
    for p, high in zip(ex_peer, higher):

        @pl.when(jnp.logical_not(high))
        def _():
            pl.semaphore_signal(barrier, inc=1, device_id=p, device_id_type=MESH)

    for load in loads[1:] + small_loads[2:]:
        load.start()

    had[...] = sign_of(jnp.bitwise_and(iota((256, 256), 0), iota((256, 256), 1)), 8).astype(BF16)
    small_loads[0].wait()
    small_loads[1].wait()
    right[...] = jnp.broadcast_to((2 * rb[...] - 1).astype(F32), (16, FF)).astype(BF16)

    def left_signs(i, carry):
        signs = (2 * lb[:, pl.ds(pl.multiple_of(i * HB, HB), HB)] - 1).astype(F32)
        left[i] = jnp.broadcast_to(signs, (HB, LANES)).T.astype(BF16)
        return carry

    left_signs(0, 0)

    def column_block(i):
        first = pl.multiple_of(i * HB, HB)
        lefts = jnp.concatenate([left[i], left[i]], axis=1)
        for p in range(8):
            x = wv[pl.ds(first, HB), p * 256:(p + 1) * 256]
            signed[p * HB:(p + 1) * HB, :] = x * lefts * right[0:1, p * 256:(p + 1) * 256]
        inner[...] = jnp.dot(signed[...], had[...], preferred_element_type=F32)
        for u in range(2):
            for r in range(HB // 16):
                parts = [inner[p * HB + r * 16:p * HB + (r + 1) * 16, u * LANES:(u + 1) * LANES] for p in range(8)]
                for t, part in enumerate(butterfly(parts)):
                    sb1[t // 4, (t % 4) * 2 + u, i, r * 16:(r + 1) * 16, :] = (part * (1.0 / math.sqrt(FF))).astype(BF16)

    def send_columns(i):
        for p in row_peer:
            push(sb1.at[0, p, i], rb1.at[0, me, i], s1_send.at[0], s1_recv.at[0], {"row": p})

    loads[0].wait()
    column_block(0)
    pl.semaphore_wait(barrier, ROWS - 1 + sum(high.astype(jnp.int32) for high in higher))
    send_columns(0)
    lax.fori_loop(1, MINE, left_signs, 0)

    def column_step(i, carry):
        pltpu.make_async_copy(w_ref.at[0, pl.ds(0, HB)], wv.at[pl.ds(0, HB)], w_sem.at[i]).wait()
        column_block(i)
        send_columns(i)
        return carry

    lax.fori_loop(1, MINE, column_step, 0)
    for i in range(MINE):
        for p in row_peer:
            push(sb1.at[1, p, i], rb1.at[1, me, i], s1_send.at[1], s1_recv.at[1], {"row": p})
    for n, (p, high) in enumerate(zip(ex_peer, higher)):

        @pl.when(high)
        def _():
            pl.semaphore_signal(here.at[n], inc=1, device_id=p, device_id_type=MESH)

    for h in range(2):
        rb1[h, me] = sb1[h, me]

    small_loads[2].wait()
    small_loads[3].wait()
    pick_a = (jnp.right_shift(iota((896, 64), 0), 4) == iota((896, 64), 1)).astype(F32).astype(BF16)
    spread = jnp.dot(pick_a, cosv[...], preferred_element_type=F32).astype(BF16)
    pick_j = (jnp.right_shift(iota((LANES, 896), 1), 4) == iota((LANES, 896), 0)).astype(F32).astype(BF16)
    mix[...] = jnp.dot(spread, pick_j, preferred_element_type=F32).astype(BF16)
    small = sign_of(
        jnp.bitwise_and(jnp.bitwise_and(iota((16, 896), 0), iota((16, 896), 1)), 15), 4
    ).astype(BF16)

    def sign_mix(a, carry):
        at = pl.ds(pl.multiple_of(a * 16, 16), 16)
        mix[at, :] = mix[at, :] * small
        return carry

    lax.fori_loop(0, BLOCKS, sign_mix, 0)
    for s in range(8):
        perm[:, s * LANES:(s + 1) * LANES] = (
            iota((1024, LANES), 0) == 8 * iota((1024, LANES), 1) + s
        ).astype(F32).astype(BF16)
    which = iota((16, 1024), 0)
    ids = jnp.zeros((16, 1024), F32)
    for h in range(2):
        ids = jnp.where(which == h, gv[:, h * 1024:(h + 1) * 1024].astype(F32), ids)
        own = gv[:, pl.ds(pl.multiple_of(h * 1024 + me * LANES, LANES), LANES)].astype(F32)
        ids = jnp.where(which == 2 + h, jnp.concatenate([own] * 8, axis=1), ids)
    gperm[...] = jnp.dot(ids.astype(BF16), perm[...], preferred_element_type=F32)

    def rotate_rows(h):
        arrived(rb1.at[h, pl.ds(0, ROWS - 1)], s1_recv.at[h])

        def mix_blocks(q, carry):
            parts = []
            for half in range(2):
                at = pl.ds(pl.multiple_of(q * 32 + half * 16, 16), 16)
                parts.append(rb1[h, :, :, at, :].reshape(896, LANES))
            out = jnp.dot(mix[...], jnp.concatenate(parts, axis=1), preferred_element_type=F32)
            mid[2 * q] = out[:, :LANES]
            mid[2 * q + 1] = out[:, LANES:]
            return carry

        lax.fori_loop(0, 4, mix_blocks, 0)

        def turn(a, peak):
            at = pl.ds(pl.multiple_of(a * 16, 16), 16)
            parts = butterfly([mid[q, at, :] for q in range(8)])
            for q, part in enumerate(parts):
                part = part * (1.0 / math.sqrt(HB))
                peak = jnp.maximum(peak, jnp.abs(part))
                rot[h, a // MINE, lax.rem(a, MINE), q * 16:(q + 1) * 16, :] = part.astype(BF16)
            return peak

        peak = lax.fori_loop(0, BLOCKS, turn, jnp.zeros((16, LANES), F32), unroll=4)
        rb2[h, me] = rot[h, me]
        return jnp.max(peak, axis=0, keepdims=True)

    def send_rows(h, blocks):
        for i in blocks:
            for p in row_peer:
                push(rot.at[h, p, i], rb2.at[h, me, i], s2_send.at[h], s2_recv.at[h, i], {"row": p})

    def to_row(slots, own, source, send, recv):
        slots[me] = own
        source[...] = own
        for p in row_peer:
            push(source, slots.at[me], send, recv, {"row": p})

    col_peak = [rotate_rows(0)]
    send_rows(0, range(0, FIRST))
    col_peak.append(rotate_rows(1))

    group_id = iota((GROUPS, LANES), 0)
    most = jnp.zeros((GROUPS, LANES), F32)
    for h in range(2):
        own = gv[:, pl.ds(pl.multiple_of(h * 1024 + me * LANES, LANES), LANES)]
        most = jnp.maximum(most, jnp.where(group_id == own, col_peak[h], 0.0))
    most = jnp.broadcast_to(jnp.max(most, axis=1, keepdims=True), (GROUPS, LANES))
    to_row(pk_r, most, pk_s, pk_send, pk_recv)
    send_rows(0, range(FIRST, MINE))

    arrived(pk_r.at[pl.ds(0, ROWS - 1)], pk_recv)
    group_peak = jnp.ones((GROUPS, LANES), F32)
    for k in range(ROWS):
        group_peak = jnp.maximum(group_peak, pk_r[k])
    small_ref[0:1, :] = jnp.sum(
        jnp.where(group_id == iota((GROUPS, LANES), 1), group_peak * 0.5, 0.0), axis=0, keepdims=True
    )
    inverse = 2.0 / group_peak
    for m in range(16):
        ids = gv[:, m * LANES:(m + 1) * LANES]
        cs_nat[m:m + 1, :] = jnp.sum(jnp.where(group_id == ids, inverse, 0.0), axis=0, keepdims=True)
    for k in range(4):
        for s in range(8):
            ids = gperm[k:k + 1, s * LANES:(s + 1) * LANES]
            cs_perm[k, s:s + 1, :] = jnp.sum(
                jnp.where(group_id.astype(F32) == ids, inverse, 0.0), axis=0, keepdims=True
            )

    def reorder(n):
        parts = []
        for h in range(2):
            blocks = [rot[h, (n * 8 + k) // MINE, (n * 8 + k) % MINE] for k in range(8)]
            parts.append(jnp.concatenate(blocks, axis=1))
        return jnp.dot(jnp.concatenate(parts, axis=0), perm[...], preferred_element_type=F32)

    def own_errors(n, total):
        block = n * 8 + jnp.right_shift(iota((8, LANES), 1), 4)
        for h in range(2):
            scales = [cs_perm[2 + h, s:s + 1, :] for s in range(8)]
            for r in range(HB // 8):
                at = slice(h * HB + r * 8, h * HB + r * 8 + 8)
                errors = lattice([ybuf[n % 2, at, s * LANES:(s + 1) * LANES] * scales[s] for s in range(8)])
                row = (block * HB + r * 8 + iota((8, LANES), 0)).astype(F32)
                total = total + errors * ((1.0 + 4.0 * (row + 0.5) / D) / 3.0)
        return total

    error = jnp.zeros((8, LANES), F32)
    ybuf[0] = reorder(0)
    for n in range(MINE):
        if n + 1 < MINE:
            ybuf[(n + 1) % 2] = reorder(n + 1)
        error = own_errors(n, error)
    to_row(e_r, error, e_s, e_send, e_recv)
    send_rows(1, range(0, MINE))

    def finish(h, start, stop):
        def step(i, carry):
            arrived(rb2.at[h, pl.ds(0, ROWS - 1), i], s2_recv.at[h, i])
            first = pl.multiple_of(i * HB, HB)

            def put_scaled(k, value):
                scaled_ref[0, pl.ds(first, HB), (h * 8 + k) * LANES:(h * 8 + k + 1) * LANES] = value

            def put_errors(r, value):
                err_ref[0, pl.ds(pl.multiple_of(first + r * 8, 8), 8), h * LANES:(h + 1) * LANES] = value

            finish_block(
                [rb2[h, k, i] for k in range(ROWS)], perm, ybuf.at[0],
                [cs_nat[h * 8 + k:h * 8 + k + 1, :] for k in range(ROWS)],
                [cs_perm[h, s:s + 1, :] for s in range(8)], put_scaled, put_errors,
            )
            return carry

        lax.fori_loop(start, stop, step, 0)

    finish(0, 0, 4)
    arrived(e_r.at[pl.ds(0, ROWS - 1)], e_recv)
    error = e_r[0]
    for k in range(1, ROWS):
        error = error + e_r[k]
    error = jnp.sum(jnp.sum(error, axis=1, keepdims=True), axis=0, keepdims=True) * (1.0 / (D * FF // 8))
    total = jnp.broadcast_to(error, (8, LANES))
    small_ref[1:2, :] = total[:1]
    meanwhile = ((0, 4, MINE), (1, 0, 1), (1, 1, 2), (1, 2, MINE - 1))
    for n, p in enumerate(ex_peer):
        t_s[n] = total

        @pl.when(jnp.logical_not(higher[n]))
        def _():
            pl.semaphore_wait(here.at[n], 1)

        push(t_s.at[n], t_r.at[n], t_send.at[n], t_recv.at[n], p)
        finish(*meanwhile[n])
        arrived(t_r.at[n], t_recv.at[n])
        total = total + t_r[n]
    small_ref[2:3, :] = total[:1] * (1.0 / PEERS)
    arrived(rb2.at[1, pl.ds(0, ROWS - 1), MINE - 1], s2_recv.at[1, MINE - 1])
    for k in range(ROWS):
        last_ref[k] = rb2[1, k, MINE - 1]

    for h in range(2):
        arrived(sb1.at[h, pl.ds(0, ROWS - 1)], s1_send.at[h])
        arrived(rot.at[h, pl.ds(0, ROWS - 1)], s2_send.at[h])
    arrived(pk_r.at[pl.ds(0, ROWS - 1)], pk_send)
    arrived(e_r.at[pl.ds(0, ROWS - 1)], e_send)
    for n in range(len(TOTAL_ORDER)):
        arrived(t_s.at[n], t_send.at[n])


def finish_kernel(
    scaled, errors, small, last, perm, cs_nat, cs_perm,
    scaled_ref, err_ref, scale_ref, expert_ref, total_ref,
    ybuf, scaled_last, err_last, scale_v, expert_v, total_v, sems,
):
    edge = (MINE - 1) * HB
    half = FF // 2
    copies = [
        pltpu.make_async_copy(scaled.at[:, pl.ds(0, edge)], scaled_ref.at[:, pl.ds(0, edge)], sems.at[0]),
        pltpu.make_async_copy(
            scaled.at[:, pl.ds(edge, HB), pl.ds(0, half)], scaled_ref.at[:, pl.ds(edge, HB), pl.ds(0, half)], sems.at[1]
        ),
        pltpu.make_async_copy(errors.at[:, pl.ds(0, edge)], err_ref.at[:, pl.ds(0, edge)], sems.at[2]),
        pltpu.make_async_copy(
            errors.at[:, pl.ds(edge, HB), pl.ds(0, LANES)], err_ref.at[:, pl.ds(edge, HB), pl.ds(0, LANES)], sems.at[3]
        ),
    ]
    for copy in copies:
        copy.start()
    scale_v[...] = small[0:1, :GROUPS]
    expert_v[...] = small[1:2, :1]
    total_v[...] = small[2:3, :1]
    for n, (src, dst) in enumerate(((scale_v, scale_ref), (expert_v, expert_ref), (total_v, total_ref))):
        copies.append(pltpu.make_async_copy(src, dst, sems.at[6 + n]))
        copies[-1].start()

    def put_scaled(k, value):
        scaled_last[0, :, k * LANES:(k + 1) * LANES] = value

    def put_errors(r, value):
        err_last[0, pl.ds(pl.multiple_of(r * 8, 8), 8), :] = value

    finish_block(
        [last[k] for k in range(ROWS)], perm, ybuf,
        [cs_nat[8 + k:9 + k, :] for k in range(ROWS)],
        [cs_perm[1, s:s + 1, :] for s in range(8)], put_scaled, put_errors,
    )
    rest = [
        pltpu.make_async_copy(scaled_last, scaled_ref.at[:, pl.ds(edge, HB), pl.ds(half, half)], sems.at[4]),
        pltpu.make_async_copy(err_last, err_ref.at[:, pl.ds(edge, HB), pl.ds(LANES, LANES)], sems.at[5]),
    ]
    for copy in rest:
        copy.start()
    for copy in copies + rest:
        copy.wait()


def body(weights, left_bits, right_bits, groups):
    vmem = pl.BlockSpec(memory_space=pltpu.VMEM)
    hbm = pl.BlockSpec(memory_space=pltpu.HBM)
    rows = MINE * HB
    dma = pltpu.SemaphoreType.DMA
    arguments = [
        pltpu.with_memory_space_constraint(x, pltpu.HBM)
        for x in (weights, left_bits, right_bits, groups, jnp.asarray(cosine_table()))
    ]
    parts = pl.pallas_call(
        rotate_kernel,
        out_shape=(
            pltpu.VMEM((1, rows, FF), BF16),
            pltpu.VMEM((1, rows, FF // 8), F32),
            pltpu.VMEM((8, LANES), F32),
            pltpu.VMEM((ROWS, HB, LANES), BF16),
            pltpu.VMEM((1024, 1024), BF16),
            pltpu.VMEM((16, LANES), F32),
            pltpu.VMEM((4, 8, LANES), F32),
        ),
        in_specs=[hbm] * 5,
        out_specs=(vmem,) * 7,
        scratch_shapes=[
            pltpu.VMEM((rows, FF), BF16),
            pltpu.VMEM((1, rows), jnp.int32),
            pltpu.VMEM((1, FF), jnp.int32),
            pltpu.VMEM((1, FF), jnp.int32),
            pltpu.VMEM((64, LANES), BF16),
            pltpu.VMEM((256, 256), BF16),
            pltpu.VMEM((896, 896), BF16),
            pltpu.VMEM((16, FF), BF16),
            pltpu.VMEM((MINE, HB, LANES), BF16),
            pltpu.VMEM((8 * HB, 256), BF16),
            pltpu.VMEM((8 * HB, 256), F32),
            pltpu.VMEM((2, ROWS, MINE, HB, LANES), BF16),
            pltpu.VMEM((2, ROWS, MINE, HB, LANES), BF16),
            pltpu.VMEM((8, 896, LANES), F32),
            pltpu.VMEM((2, ROWS, MINE, HB, LANES), BF16),
            pltpu.VMEM((2, ROWS, MINE, HB, LANES), BF16),
            pltpu.VMEM((2, 2 * HB, 1024), F32),
            pltpu.VMEM((16, 1024), F32),
            pltpu.VMEM((GROUPS, LANES), F32),
            pltpu.VMEM((ROWS, GROUPS, LANES), F32),
            pltpu.VMEM((8, LANES), F32),
            pltpu.VMEM((ROWS, 8, LANES), F32),
            pltpu.VMEM((len(TOTAL_ORDER), 8, LANES), F32),
            pltpu.VMEM((len(TOTAL_ORDER), 8, LANES), F32),
            pltpu.SemaphoreType.REGULAR((len(TOTAL_ORDER),)),
            dma((MINE,)),
            dma((4,)),
            dma((2,)),
            dma((2,)),
            dma((2,)),
            dma((2, MINE)),
            dma,
            dma,
            dma,
            dma,
            dma((len(TOTAL_ORDER),)),
            dma((len(TOTAL_ORDER),)),
        ],
        compiler_params=pltpu.CompilerParams(
            collective_id=0, has_side_effects=True, vmem_limit_bytes=VMEM_LIMIT
        ),
        name="rotate",
    )(*arguments)
    scaled, errors, scales, expert_error, total_error = pl.pallas_call(
        finish_kernel,
        out_shape=(
            jax.ShapeDtypeStruct((1, rows, FF), BF16),
            jax.ShapeDtypeStruct((1, rows, FF // 8), F32),
            jax.ShapeDtypeStruct((1, GROUPS), F32),
            jax.ShapeDtypeStruct((1, 1), F32),
            jax.ShapeDtypeStruct((1, 1), F32),
        ),
        in_specs=[vmem] * 7,
        out_specs=(hbm,) * 5,
        scratch_shapes=[
            pltpu.VMEM((HB, 1024), F32),
            pltpu.VMEM((1, HB, FF // 2), BF16),
            pltpu.VMEM((1, HB, LANES), F32),
            pltpu.VMEM((1, GROUPS), F32),
            pltpu.VMEM((1, 1), F32),
            pltpu.VMEM((1, 1), F32),
            dma((9,)),
        ],
        compiler_params=pltpu.CompilerParams(vmem_limit_bytes=8 * 2**20),
        name="finish",
    )(*parts)
    return scaled, errors, scales, expert_error.reshape(1), total_error.reshape(())


def solution(mesh):
    placed = (P("expert", "row", None), P("expert", "row"), P("expert", None), P("expert", None))
    return jax.shard_map(
        body,
        mesh=mesh,
        in_specs=placed,
        out_specs=(
            P("expert", "row", None),
            P("expert", "row", None),
            P("expert", None),
            P("expert"),
            P(),
        ),
        check_vma=False,
    )
```
